128 devices in a mesh: lat: 8 (over z, core), lon: 16 (over y, x).
Axes of the slice: x: 4, y: 4, z: 4, core: 2. Of those that a mesh axis runs over, the one named last changes fastest.
Arguments:
- increments: bfloat16 [262144, 3, 128], P(('lat', 'lon')), may hold values from -6 to 6
- cotangent: bfloat16 [262144, 128], P(('lat', 'lon')), may hold values from -6 to 6
- owner_perm: int32 [128, 2048], P(('lat', 'lon')), may hold values from 0 to 2047, each once within a row
- coarse_index: int32 [2, 131072], P(None, ('lat', 'lon')), may hold values from 0 to 2047
- coarse_weight: float32 [131072], P(('lat', 'lon')), may hold values from 0.2 to 0.8
- back_index: int32 [2, 262144], P(None, ('lat', 'lon')), may hold values from 0 to 1023
- back_weight: float32 [262144], P(('lat', 'lon')), may hold values from 0.2 to 0.8
- lw_scale: float32 [16, 131072], P(None, ('lat', 'lon')), may hold values from 0.1 to 1
- sw_scale: float32 [14, 131072], P(None, ('lat', 'lon')), may hold values from 0.2 to 2
- sunlit: int32 [131072], P(('lat', 'lon')), may hold values from 0 to 1, as said below
- lw_table: bfloat16 [16, 3, 128, 128], P(None, None, 'lon'), may hold values from -0.3125 to 0.3125
- sw_table: bfloat16 [14, 3, 128, 128], P(None, None, 'lon'), may hold values from -0.3125 to 0.3125
Outputs:
- tendency: bfloat16 [262144, 128], P(('lat', 'lon'))
- gradient: bfloat16 [262144, 3, 128], P(('lat', 'lon'))
The draws below stay inside these ranges and needn't reach their ends.
Inputs may be any that keep to these rules, and one draw needn't show every extreme that they name: In each device's block of 1024 radiation columns at most 640 are sunlit, and some device has exactly 640.
All inputs are finite; a program needn't handle non-finite values.
Results may differ from the reference program's by a relative error of at most 0.014.
Values may be sent and summed in bfloat16 or wider, within the bound.
No kernel may reach another device: no remote copies, remote signals or barrier semaphores. Data moves between devices by JAX's collectives and lax.ppermute only.
A program may use at most 64 MiB of HBM per device.

```python
import math
import jax
import jax.numpy as jnp
from jax import lax

COLS_DEV = 2048
LEV = 128
VARS = 3
BANDS_LW = 16
BANDS_SW = 14
RC_DEV = 1024
SUNMAX = 640
COLS = 262144
RCOLS = 131072
N_LAT = 8
N_LON = 16
DEVICES = 128


def draw_sunlit(key, part):
    key_count, key_full, key_order = jax.random.split(key, 3)
    counts = jax.random.randint(key_count, (DEVICES,), SUNMAX // 8, SUNMAX + 1)
    chosen = jax.random.randint(key_full, (), 0, DEVICES)
    counts = jnp.where(jnp.arange(DEVICES) == chosen, SUNMAX, counts)
    scores = jax.random.randint(key_order, (DEVICES, RC_DEV), 0, 1 << 18) * RC_DEV + jnp.arange(RC_DEV, dtype=jnp.int32)[None, :]
    ranks = jnp.argsort(jnp.argsort(scores, axis=1), axis=1)
    return (ranks < counts[:, None]).astype(jnp.int32).reshape(-1)


def place_ends(values, own_key, smallest, top_value):
    dims = values.shape
    spot = [jax.random.randint(jax.random.fold_in(own_key, axis), (), 0, dims[axis]) for axis in range(len(dims))]
    values = values.at[tuple(spot)].set(smallest)
    longest = dims.index(max(dims))
    spot[longest] = (spot[longest] + 1) % dims[longest]
    return values.at[tuple(spot)].set(top_value)


def block_levels(own_key, shape, cuts, low, high):
    factor_of, own = 1.0, jax.random.fold_in(own_key, 6)
    for axis_at, shards_of in cuts:
        heights = jnp.exp(jax.random.uniform(jax.random.fold_in(own, axis_at), (shards_of,), jnp.float32, low / len(cuts), high / len(cuts)))
        factor_of = factor_of * jnp.repeat(heights, shape[axis_at] // shards_of).reshape([-1 if axis == axis_at else 1 for axis in range(len(shape))])
    return factor_of


def scatter_about(stream_key, shape, deviation, bound, cuts=(), kind=jnp.bfloat16):
    array = jax.random.normal(stream_key, shape, jnp.float32) * deviation
    if len(cuts) > 0:
        array = block_levels(stream_key, shape, cuts, -0.22, 0.18) * array
    return jnp.clip(array, min=-bound, max=bound).astype(kind)


def setup_inputs(seed: int = 0) -> dict:
    splits = jax.random.split(jax.random.key(seed), 13)
    increments = scatter_about(splits[0], (COLS, VARS, LEV), 1.0, 6.0, ((0, 128),))
    cotangent = scatter_about(splits[1], (COLS, LEV), 1.0, 6.0, ((0, 128),))
    owner_perm = jax.vmap(lambda own: jax.random.permutation(own, COLS_DEV))(jax.random.split(splits[2], DEVICES)).reshape((DEVICES, COLS_DEV)).astype(jnp.int32)
    coarse_index = place_ends(jax.random.randint(splits[3], (2, RCOLS), 0, COLS_DEV), jax.random.fold_in(splits[3], 1), 0, COLS_DEV - 1).astype(jnp.int32)
    coarse_weight = jnp.clip(0.2 + 0.6 * jax.random.uniform(splits[4], (RCOLS,), jnp.float32) ** block_levels(splits[4], (RCOLS,), ((0, 128),), -0.2, 0.2), 0.2, 0.8)
    back_index = place_ends(jax.random.randint(splits[5], (2, COLS), 0, RC_DEV), jax.random.fold_in(splits[5], 1), 0, RC_DEV - 1).astype(jnp.int32)
    back_weight = jnp.clip(0.2 + 0.6 * jax.random.uniform(splits[6], (COLS,), jnp.float32) ** block_levels(splits[6], (COLS,), ((0, 128),), -0.2, 0.2), 0.2, 0.8)
    lw_scale = jnp.clip(jnp.exp(math.log(1.0) - 2.3025851 * jax.random.uniform(splits[7], (BANDS_LW, RCOLS), jnp.float32) ** block_levels(splits[7], (BANDS_LW, RCOLS), ((1, 128),), -0.2, 0.2)), 0.1, 1.0)
    sw_scale = jnp.clip(jnp.exp(math.log(2.0) - 2.3025851 * jax.random.uniform(splits[8], (BANDS_SW, RCOLS), jnp.float32) ** block_levels(splits[8], (BANDS_SW, RCOLS), ((1, 128),), -0.2, 0.2)), 0.2, 2.0)
    sunlit = draw_sunlit(jax.random.fold_in(splits[12], 71), 0)
    lw_table = scatter_about(splits[10], (BANDS_LW, VARS, LEV, LEV), (VARS * LEV) ** -0.5, 0.3125, ((2, 16),))
    sw_table = scatter_about(splits[11], (BANDS_SW, VARS, LEV, LEV), (VARS * LEV) ** -0.5, 0.3125, ((2, 16),))
    return {"increments": increments, "cotangent": cotangent, "owner_perm": owner_perm, "coarse_index": coarse_index, "coarse_weight": coarse_weight, "back_index": back_index, "back_weight": back_weight, "lw_scale": lw_scale, "sw_scale": sw_scale, "sunlit": sunlit, "lw_table": lw_table, "sw_table": sw_table}


def band_sum(coarse, band_table, band_scale):
    product = jnp.einsum("rc,bck->rbk", coarse.astype(jnp.float32), band_table.astype(jnp.float32))
    return jnp.einsum("br,rbk->rk", band_scale, product)


def band_adjoint(adjoint_coarse, band_table, band_scale):
    lifted = (band_scale.T[:, :, None] * adjoint_coarse[:, None, :]).astype(jnp.bfloat16)
    lifted = lax.optimization_barrier(lifted)
    return jnp.einsum("rbk,bck->rc", lifted.astype(jnp.float32), band_table.astype(jnp.float32))


def radiate(fields, cot_rad, coarse_index, coarse_weight, back_index, back_weight, lw_scale, sw_scale, sunlit, lw_bands, sw_bands):
    row_count = coarse_weight.shape[0]
    col_count = back_weight.shape[0]
    flat_rows = fields.reshape(col_count, -1)
    first = flat_rows[coarse_index[0]].astype(jnp.float32)
    second = flat_rows[coarse_index[1]].astype(jnp.float32)
    coarse = (coarse_weight[:, None] * first + (1.0 - coarse_weight)[:, None] * second).astype(jnp.bfloat16)
    sw_weight = sw_scale * sunlit.astype(jnp.float32)[None, :]
    heating = band_sum(coarse, lw_bands, lw_scale) + band_sum(coarse, sw_bands, sw_weight)
    tendency_rad = (back_weight[:, None] * heating[back_index[0]] + (1.0 - back_weight)[:, None] * heating[back_index[1]]).astype(jnp.bfloat16)
    cot_float = cot_rad.astype(jnp.float32)
    adjoint_coarse = jax.ops.segment_sum(
        jnp.concatenate([back_weight[:, None] * cot_float, (1.0 - back_weight)[:, None] * cot_float]),
        jnp.concatenate([back_index[0], back_index[1]]), num_segments=row_count)
    adjoint_rows = band_adjoint(adjoint_coarse, lw_bands, lw_scale) + band_adjoint(adjoint_coarse, sw_bands, sw_weight)
    gradient_rad = jax.ops.segment_sum(
        jnp.concatenate([coarse_weight[:, None] * adjoint_rows, (1.0 - coarse_weight)[:, None] * adjoint_rows]),
        jnp.concatenate([coarse_index[0], coarse_index[1]]), num_segments=col_count).astype(jnp.bfloat16)
    return tendency_rad, gradient_rad.reshape(fields.shape)


def pick_rows(values, order_map):
    return values[order_map]


def restore_rows(values, order_map):
    return jnp.zeros_like(values).at[order_map].set(values)


def reference(increments, cotangent, owner_perm, coarse_index, coarse_weight, back_index, back_weight, lw_scale, sw_scale, sunlit, lw_table, sw_table):
    device_count = N_LAT * N_LON
    segment = COLS_DEV // device_count

    def relay(values):
        rest = values.shape[2:]
        return values.reshape((device_count, device_count, segment) + rest).swapaxes(0, 1).reshape((device_count, COLS_DEV) + rest)

    fields_model = increments.reshape(device_count, COLS_DEV, VARS, LEV)
    cot_model = cotangent.reshape(device_count, COLS_DEV, LEV)
    fields = relay(jax.vmap(pick_rows)(fields_model, owner_perm))
    cot_rad = relay(jax.vmap(pick_rows)(cot_model, owner_perm))
    coarse_dev = coarse_index.reshape(2, device_count, RC_DEV).swapaxes(0, 1)
    coarse_wdev = coarse_weight.reshape(device_count, RC_DEV)
    back_dev = back_index.reshape(2, device_count, COLS_DEV).swapaxes(0, 1)
    back_wdev = back_weight.reshape(device_count, COLS_DEV)
    lw_dev = lw_scale.reshape(BANDS_LW, device_count, RC_DEV).swapaxes(0, 1)
    sw_dev = sw_scale.reshape(BANDS_SW, device_count, RC_DEV).swapaxes(0, 1)
    sun_dev = sunlit.reshape(device_count, RC_DEV)
    lw_bands = lw_table.reshape(BANDS_LW, VARS * LEV, LEV)
    sw_bands = sw_table.reshape(BANDS_SW, VARS * LEV, LEV)

    def one_device(item):
        return radiate(item[0], item[1], item[2], item[3], item[4], item[5], item[6], item[7], item[8], lw_bands, sw_bands)

    tendency_rad, gradient_rad = lax.map(one_device, (fields, cot_rad, coarse_dev, coarse_wdev, back_dev, back_wdev, lw_dev, sw_dev, sun_dev))
    tendency = jax.vmap(restore_rows)(relay(tendency_rad), owner_perm)
    gradient = jax.vmap(restore_rows)(relay(gradient_rad), owner_perm)
    return tendency.reshape(COLS, LEV), gradient.reshape(COLS, VARS, LEV)
```

```python
import functools

import jax
import jax.numpy as jnp
from jax import lax
from jax.experimental import pallas as pl
from jax.experimental.pallas import tpu as pltpu
from jax.sharding import PartitionSpec as P

ALL = ("lat", "lon")
F32 = jnp.float32
BF16 = jnp.bfloat16


def columns(row, start, count):
    piece = row[:, start : start + count]
    return jnp.transpose(jnp.broadcast_to(piece, (128, count)))


def wide(column, width):
    return jnp.concatenate([column] * (width // 128), axis=1)


def pick_kernel(planes, perm_ref, *refs):
    sources, out_ref = refs[:-1], refs[-1]
    rows = out_ref.shape[0]
    total = perm_ref.shape[1]
    start = pl.multiple_of(pl.program_id(0) * rows, rows)
    index = jnp.transpose(jnp.broadcast_to(perm_ref[:, pl.ds(start, rows)], (128, rows)))
    lanes = lax.broadcasted_iota(jnp.int32, (rows, total), 1)
    hot = (wide(index, total) == lanes).astype(F32).astype(BF16)
    pieces = []
    for ref in sources:
        if len(ref.shape) == 3:
            pieces.extend(ref[v] for v in range(ref.shape[0]))
        else:
            pieces.append(ref[...])
    data = pieces[0] if len(pieces) == 1 else jnp.concatenate(pieces, axis=1)
    out_ref[...] = jnp.dot(hot, data, preferred_element_type=F32).astype(BF16)


def full(shape):
    return pl.BlockSpec(shape, lambda *_: (0,) * len(shape))


def cost(flops, nbytes):
    return pl.CostEstimate(flops=flops, bytes_accessed=nbytes, transcendentals=0)


def pick(perm, *sources):
    total = perm.shape[1]
    width = sum(s.shape[0] * s.shape[2] if s.ndim == 3 else s.shape[1] for s in sources)
    rows = 512
    return pl.pallas_call(
        functools.partial(pick_kernel, None),
        grid=(total // rows,),
        in_specs=[full(perm.shape)] + [full(s.shape) for s in sources],
        out_specs=pl.BlockSpec((rows, width), lambda i: (i, 0)),
        out_shape=jax.ShapeDtypeStruct((total, width), BF16),
        cost_estimate=cost(2 * total * total * width, 4 * total * width),
        name="pick",
    )(perm, *sources)


def restore_kernel(perm_ref, data_ref, out_ref):
    rows = out_ref.shape[-2]
    total = perm_ref.shape[1]
    start = pl.program_id(0) * rows
    targets = lax.broadcasted_iota(jnp.int32, (rows, total), 0) + start
    hot = (jnp.broadcast_to(perm_ref[...], (rows, total)) == targets).astype(F32).astype(BF16)
    got = jnp.dot(hot, data_ref[...], preferred_element_type=F32).astype(BF16)
    if len(out_ref.shape) == 3:
        for v in range(out_ref.shape[0]):
            out_ref[v] = got[:, v * 128 : (v + 1) * 128]
    else:
        out_ref[...] = got


def restore(perm, data):
    total, width = data.shape
    rows = 512
    if width > 128:
        planes = width // 128
        out_spec = pl.BlockSpec((planes, rows, 128), lambda i: (0, i, 0))
        out_shape = jax.ShapeDtypeStruct((planes, total, 128), BF16)
    else:
        out_spec = pl.BlockSpec((rows, width), lambda i: (i, 0))
        out_shape = jax.ShapeDtypeStruct((total, width), BF16)
    return pl.pallas_call(
        restore_kernel,
        grid=(total // rows,),
        in_specs=[full(perm.shape), full(data.shape)],
        out_specs=out_spec,
        out_shape=out_shape,
        cost_estimate=cost(2 * total * total * width, 4 * total * width),
        name="restore",
    )(perm, data)


def two_hot_columns(first, second, share, width):
    rows = first.shape[0]
    lanes = lax.broadcasted_iota(jnp.int32, (rows, width), 1)
    one = jnp.where(wide(first, width) == lanes, wide(share, width), 0.0)
    two = jnp.where(wide(second, width) == lanes, wide(1.0 - share, width), 0.0)
    return (one + two).astype(BF16)


def two_hot_rows(first, second, share, rows, start):
    width = first.shape[1]
    targets = lax.broadcasted_iota(jnp.int32, (rows, width), 0) + start
    one = jnp.where(jnp.broadcast_to(first, (rows, width)) == targets, share, 0.0)
    two = jnp.where(jnp.broadcast_to(second, (rows, width)) == targets, 1.0 - share, 0.0)
    return (one + two).astype(BF16)


def scale_columns(scale_ref, start, rows):
    return jnp.transpose(scale_ref[:, pl.ds(start, rows)])


def adjoint_kernel(
    cot_ref, bidx_ref, bw_ref, cidx_ref, cw_ref, scale_ref, ta_ref, tb_ref, out_ref, adj_ref, rows_ref
):
    row_count = adj_ref.shape[0]
    col_count = out_ref.shape[0]
    block = 256
    bands = ta_ref.shape[0]

    def spread(i, carry):
        start = pl.multiple_of(i * block, block)
        table = two_hot_rows(bidx_ref[0:1, :], bidx_ref[1:2, :], bw_ref[...], block, start)
        adj = jnp.dot(table, cot_ref[...], preferred_element_type=F32)
        scales = scale_columns(scale_ref, start, block)
        lifted = [
            (jnp.broadcast_to(scales[:, b : b + 1], (block, 128)) * adj).astype(BF16)
            for b in range(2 * bands)
        ]
        weights = [ta_ref[b] for b in range(bands)] + [tb_ref[b] for b in range(bands)]
        rows_ref[pl.ds(start, block), :] = lax.dot_general(
            jnp.concatenate(lifted, axis=1),
            jnp.concatenate(weights, axis=1),
            (((1,), (1,)), ((), ())),
            preferred_element_type=F32,
        ).astype(BF16)
        return carry

    lax.fori_loop(0, row_count // block, spread, 0)

    def scatter(i, carry):
        start = pl.multiple_of(i * block, block)
        table = two_hot_rows(cidx_ref[0:1, :], cidx_ref[1:2, :], cw_ref[...], block, start)
        out_ref[pl.ds(start, block), :] = jnp.dot(
            table, rows_ref[...], preferred_element_type=F32
        ).astype(BF16)
        return carry

    lax.fori_loop(0, col_count // block, scatter, 0)


def adjoint(cot, bidx, bw, cidx, cw, scale, ta, tb):
    col_count = cot.shape[0]
    row_count = cw.shape[1]
    width = ta.shape[1]
    return pl.pallas_call(
        adjoint_kernel,
        out_shape=jax.ShapeDtypeStruct((col_count, width), BF16),
        scratch_shapes=[
            pltpu.VMEM((row_count, 128), F32),
            pltpu.VMEM((row_count, width), BF16),
        ],
        cost_estimate=cost(2 * row_count * 128 * 30 * width * 2, 8 * 1024 * 1024),
        name="adjoint",
    )(cot, bidx, bw, cidx, cw, scale, ta, tb)


def forward_kernel(
    fields_ref, bidx_ref, bw_ref, cidx_ref, cw_ref, scale_ref, ta_ref, tb_ref, out_ref, heat_ref
):
    row_count = heat_ref.shape[0]
    col_count = out_ref.shape[0]
    block = 256
    bands = ta_ref.shape[0]

    def band(i, carry):
        start = pl.multiple_of(i * block, block)
        get = lambda ref, k: jnp.transpose(
            jnp.broadcast_to(ref[k : k + 1, pl.ds(start, block)], (128, block))
        )
        table = two_hot_columns(get(cidx_ref, 0), get(cidx_ref, 1), get(cw_ref, 0), col_count)
        coarse = jnp.dot(table, fields_ref[...], preferred_element_type=F32).astype(BF16)
        scales = scale_columns(scale_ref, start, block)
        weights = [ta_ref[b] for b in range(bands)] + [tb_ref[b] for b in range(bands)]
        heat = jnp.zeros((block, 128), F32)
        for pair in range(bands):
            both = jnp.concatenate(weights[2 * pair : 2 * pair + 2], axis=1)
            product = jnp.dot(coarse, both, preferred_element_type=F32)
            for half in range(2):
                b = 2 * pair + half
                heat = heat + jnp.broadcast_to(scales[:, b : b + 1], (block, 128)) * product[
                    :, half * 128 : (half + 1) * 128
                ]
        heat_ref[pl.ds(start, block), :] = heat.astype(BF16)
        return carry

    lax.fori_loop(0, row_count // block, band, 0)

    def back(i, carry):
        start = pl.multiple_of(i * block, block)
        get = lambda ref, k: jnp.transpose(
            jnp.broadcast_to(ref[k : k + 1, pl.ds(start, block)], (128, block))
        )
        table = two_hot_columns(get(bidx_ref, 0), get(bidx_ref, 1), get(bw_ref, 0), row_count)
        out_ref[pl.ds(start, block), :] = jnp.dot(
            table, heat_ref[...], preferred_element_type=F32
        ).astype(BF16)
        return carry

    lax.fori_loop(0, col_count // block, back, 0)


def forward(fields, bidx, bw, cidx, cw, scale, ta, tb):
    col_count = fields.shape[0]
    row_count = cw.shape[1]
    return pl.pallas_call(
        forward_kernel,
        out_shape=jax.ShapeDtypeStruct((col_count, 128), BF16),
        scratch_shapes=[pltpu.VMEM((row_count, 128), BF16)],
        cost_estimate=cost(2 * row_count * 128 * 30 * fields.shape[1] * 2, 8 * 1024 * 1024),
        name="forward",
    )(fields, bidx, bw, cidx, cw, scale, ta, tb)


def exchange(values, axes):
    return lax.all_to_all(values, axes, split_axis=0, concat_axis=0, tiled=True)


def local(
    increments,
    cotangent,
    owner_perm,
    coarse_index,
    coarse_weight,
    back_index,
    back_weight,
    lw_scale,
    sw_scale,
    sunlit,
    lw_table,
    sw_table,
):
    lat, lon = lax.axis_size("lat"), lax.axis_size("lon")
    core = lax.rem(lax.axis_index("lat"), 2)
    table = jnp.concatenate([lw_table, sw_table], axis=0)
    bands, variables, depth, levels = table.shape
    half = bands // 2
    mine = lax.dynamic_slice_in_dim(table, core * half, half, axis=0)
    mine = jnp.broadcast_to(mine[None], (lon,) + mine.shape)
    got = exchange(mine, ("lon",))
    got = got.transpose(1, 2, 0, 3, 4).reshape(half, variables * lon * depth, levels)
    partner = [(a, a + 1 - 2 * (a % 2)) for a in range(lat)]
    other = lax.ppermute(got, "lat", partner)
    scale = jnp.concatenate([lw_scale, sw_scale * sunlit.astype(F32)[None, :]], axis=0)
    scale = jnp.where(core == 0, scale, jnp.roll(scale, half, axis=0))
    scale = jnp.pad(scale, ((0, 2), (0, 0)))

    cw = coarse_weight[None]
    bw = back_weight[None]
    planes = increments.transpose(1, 0, 2)
    cot_rad = exchange(pick(owner_perm, cotangent), ALL)
    fields = exchange(pick(owner_perm, planes), ALL)
    gradient_rad = adjoint(cot_rad, back_index, bw, coarse_index, cw, scale, got, other)
    back_gradient = exchange(gradient_rad, ALL)
    tendency_rad = forward(fields, back_index, bw, coarse_index, cw, scale, got, other)
    back_tendency = exchange(tendency_rad, ALL)
    gradient = restore(owner_perm, back_gradient).transpose(1, 0, 2)
    tendency = restore(owner_perm, back_tendency)
    return (tendency, gradient)


def solution(mesh):
    in_specs = (
        P(ALL, None, None),
        P(ALL, None),
        P(ALL, None),
        P(None, ALL),
        P(ALL),
        P(None, ALL),
        P(ALL),
        P(None, ALL),
        P(None, ALL),
        P(ALL),
        P(None, None, "lon", None),
        P(None, None, "lon", None),
    )
    out_specs = (P(ALL, None), P(ALL, None, None))
    return jax.shard_map(local, mesh=mesh, in_specs=in_specs, out_specs=out_specs, check_vma=False)
```

```python
import functools

import jax
import jax.numpy as jnp
from jax import lax
from jax.experimental import pallas as pl
from jax.experimental.pallas import tpu as pltpu
from jax.sharding import PartitionSpec as P

ALL = ("lat", "lon")
F32 = jnp.float32
BF16 = jnp.bfloat16


def columns(row, start, count):
    piece = row[:, start : start + count]
    return jnp.transpose(jnp.broadcast_to(piece, (128, count)))


def wide(column, width):
    return jnp.concatenate([column] * (width // 128), axis=1)


def pick_kernel(planes, perm_ref, *refs):
    sources, out_ref = refs[:-1], refs[-1]
    rows = out_ref.shape[0]
    total = perm_ref.shape[1]
    start = pl.multiple_of(pl.program_id(0) * rows, rows)
    index = jnp.transpose(jnp.broadcast_to(perm_ref[:, pl.ds(start, rows)], (128, rows)))
    lanes = lax.broadcasted_iota(jnp.int32, (rows, total), 1)
    hot = (wide(index, total) == lanes).astype(F32).astype(BF16)
    pieces = []
    for ref in sources:
        if len(ref.shape) == 3:
            pieces.extend(ref[v] for v in range(ref.shape[0]))
        else:
            pieces.append(ref[...])
    data = pieces[0] if len(pieces) == 1 else jnp.concatenate(pieces, axis=1)
    out_ref[...] = jnp.dot(hot, data, preferred_element_type=F32).astype(BF16)


def full(shape):
    return pl.BlockSpec(shape, lambda *_: (0,) * len(shape))


def cost(flops, nbytes):
    return pl.CostEstimate(flops=flops, bytes_accessed=nbytes, transcendentals=0)


def pick(perm, *sources):
    total = perm.shape[1]
    width = sum(s.shape[0] * s.shape[2] if s.ndim == 3 else s.shape[1] for s in sources)
    rows = 512
    return pl.pallas_call(
        functools.partial(pick_kernel, None),
        grid=(total // rows,),
        in_specs=[full(perm.shape)] + [full(s.shape) for s in sources],
        out_specs=pl.BlockSpec((rows, width), lambda i: (i, 0)),
        out_shape=jax.ShapeDtypeStruct((total, width), BF16),
        cost_estimate=cost(2 * total * total * width, 4 * total * width),
        name="pick",
    )(perm, *sources)


def restore_kernel(perm_ref, data_ref, planes_ref, last_ref):
    rows = last_ref.shape[0]
    total = perm_ref.shape[1]
    start = pl.program_id(0) * rows
    targets = lax.broadcasted_iota(jnp.int32, (rows, total), 0) + start
    hot = (jnp.broadcast_to(perm_ref[...], (rows, total)) == targets).astype(F32).astype(BF16)
    got = jnp.dot(hot, data_ref[...], preferred_element_type=F32).astype(BF16)
    planes = planes_ref.shape[0]
    for v in range(planes):
        planes_ref[v] = got[:, v * 128 : (v + 1) * 128]
    last_ref[...] = got[:, planes * 128 :]


def restore(perm, data):
    total, width = data.shape
    rows = 512
    planes = width // 128 - 1
    return pl.pallas_call(
        restore_kernel,
        grid=(total // rows,),
        in_specs=[full(perm.shape), full(data.shape)],
        out_specs=[
            pl.BlockSpec((planes, rows, 128), lambda i: (0, i, 0)),
            pl.BlockSpec((rows, 128), lambda i: (i, 0)),
        ],
        out_shape=[
            jax.ShapeDtypeStruct((planes, total, 128), BF16),
            jax.ShapeDtypeStruct((total, 128), BF16),
        ],
        cost_estimate=cost(2 * total * total * width, 4 * total * width),
        name="restore",
    )(perm, data)


def two_hot_columns(first, second, share, width):
    rows = first.shape[0]
    lanes = lax.broadcasted_iota(jnp.int32, (rows, width), 1)
    one = jnp.where(wide(first, width) == lanes, wide(share, width), 0.0)
    two = jnp.where(wide(second, width) == lanes, wide(1.0 - share, width), 0.0)
    return (one + two).astype(BF16)


def two_hot_rows(first, second, share, rows, start):
    width = first.shape[1]
    targets = lax.broadcasted_iota(jnp.int32, (rows, width), 0) + start
    one = jnp.where(jnp.broadcast_to(first, (rows, width)) == targets, share, 0.0)
    two = jnp.where(jnp.broadcast_to(second, (rows, width)) == targets, 1.0 - share, 0.0)
    return (one + two).astype(BF16)


def scale_columns(scale_ref, start, rows):
    return jnp.transpose(scale_ref[:, pl.ds(start, rows)])


def main_kernel(
    data_ref, bidx_ref, bw_ref, cidx_ref, cw_ref, scale_ref, ta_ref, tb_ref, out_ref, rows_ref, heat_ref
):
    row_count = rows_ref.shape[0]
    col_count = out_ref.shape[0]
    block = 256
    bands = ta_ref.shape[0]
    width = rows_ref.shape[1]

    def column(ref, k, start):
        return jnp.transpose(jnp.broadcast_to(ref[k : k + 1, pl.ds(start, block)], (128, block)))

    def radiate(i, carry):
        start = pl.multiple_of(i * block, block)
        weights = [ta_ref[b] for b in range(bands)] + [tb_ref[b] for b in range(bands)]
        scales = jnp.transpose(scale_ref[:, pl.ds(start, block)])
        table = two_hot_rows(bidx_ref[0:1, :], bidx_ref[1:2, :], bw_ref[...], block, start)
        adj = jnp.dot(table, data_ref[:, width:], preferred_element_type=F32)
        lifted = [
            (jnp.broadcast_to(scales[:, b : b + 1], (block, 128)) * adj).astype(BF16)
            for b in range(2 * bands)
        ]
        rows_ref[pl.ds(start, block), :] = lax.dot_general(
            jnp.concatenate(lifted, axis=1),
            jnp.concatenate(weights, axis=1),
            (((1,), (1,)), ((), ())),
            preferred_element_type=F32,
        ).astype(BF16)
        table = two_hot_columns(
            column(cidx_ref, 0, start), column(cidx_ref, 1, start), column(cw_ref, 0, start), col_count
        )
        coarse = jnp.dot(table, data_ref[:, :width], preferred_element_type=F32).astype(BF16)
        heat = jnp.zeros((block, 128), F32)
        for pair in range(bands):
            both = jnp.concatenate(weights[2 * pair : 2 * pair + 2], axis=1)
            product = jnp.dot(coarse, both, preferred_element_type=F32)
            for part in range(2):
                b = 2 * pair + part
                heat = heat + jnp.broadcast_to(scales[:, b : b + 1], (block, 128)) * product[
                    :, part * 128 : (part + 1) * 128
                ]
        heat_ref[pl.ds(start, block), :] = heat.astype(BF16)
        return carry

    lax.fori_loop(0, row_count // block, radiate, 0)

    def scatter(i, carry):
        start = pl.multiple_of(i * block, block)
        table = two_hot_rows(cidx_ref[0:1, :], cidx_ref[1:2, :], cw_ref[...], block, start)
        out_ref[pl.ds(start, block), :width] = jnp.dot(
            table, rows_ref[...], preferred_element_type=F32
        ).astype(BF16)
        table = two_hot_columns(
            column(bidx_ref, 0, start), column(bidx_ref, 1, start), column(bw_ref, 0, start), row_count
        )
        out_ref[pl.ds(start, block), width:] = jnp.dot(
            table, heat_ref[...], preferred_element_type=F32
        ).astype(BF16)
        return carry

    lax.fori_loop(0, col_count // block, scatter, 0)


def radiation(data, bidx, bw, cidx, cw, scale, ta, tb):
    col_count = data.shape[0]
    row_count = cw.shape[1]
    width = ta.shape[1]
    return pl.pallas_call(
        main_kernel,
        out_shape=jax.ShapeDtypeStruct((col_count, width + 128), BF16),
        scratch_shapes=[
            pltpu.VMEM((row_count, width), BF16),
            pltpu.VMEM((row_count, 128), BF16),
        ],
        cost_estimate=cost(2 * row_count * 128 * 30 * width * 4, 8 * 1024 * 1024),
        name="radiation",
    )(data, bidx, bw, cidx, cw, scale, ta, tb)


def gather_four(block, stride):
    lon = lax.axis_size("lon")
    place = lax.rem(lax.axis_index("lon") // stride, 4)
    size = block.shape[0]
    out = jnp.zeros((4 * size,) + block.shape[1:], block.dtype)
    got = [block]
    for shift in (1, 3, 2):
        pairs = []
        for a in range(lon):
            at = a // stride % 4
            pairs.append((a, a + ((at + shift) % 4 - at) * stride))
        got.append(lax.ppermute(block, "lon", pairs))
    for shift, piece in zip((0, 1, 3, 2), got):
        out = lax.dynamic_update_slice_in_dim(
            out, piece, lax.rem(place + 4 - shift, 4) * size, axis=0
        )
    return out


def exchange(values, axes):
    return lax.all_to_all(values, axes, split_axis=0, concat_axis=0, tiled=True)


def local(
    increments,
    cotangent,
    owner_perm,
    coarse_index,
    coarse_weight,
    back_index,
    back_weight,
    lw_scale,
    sw_scale,
    sunlit,
    lw_table,
    sw_table,
):
    lat = lax.axis_size("lat")
    core = lax.rem(lax.axis_index("lat"), 2)
    table = jnp.concatenate([lw_table, sw_table], axis=0)
    bands, variables, depth, levels = table.shape
    half = bands // 2
    mine = lax.dynamic_slice_in_dim(table, core * half, half, axis=0)
    column = gather_four(mine[None], 1)
    whole = gather_four(column, 4)
    partner = [(a, a + 1 - 2 * (a % 2)) for a in range(lat)]
    other = lax.ppermute(whole, "lat", partner)
    mine, other = (
        t.transpose(1, 2, 0, 3, 4).reshape(half, -1, levels) for t in (whole, other)
    )
    scale = jnp.concatenate([lw_scale, sw_scale * sunlit.astype(F32)[None, :]], axis=0)
    scale = jnp.where(core == 0, scale, jnp.roll(scale, half, axis=0))
    scale = jnp.pad(scale, ((0, 2), (0, 0)))

    cw = coarse_weight[None]
    bw = back_weight[None]
    planes = increments.transpose(1, 0, 2)
    data = exchange(pick(owner_perm, planes, cotangent), ALL)
    back = radiation(data, back_index, bw, coarse_index, cw, scale, mine, other)
    back = exchange(back, ALL)
    gradient, tendency = restore(owner_perm, back)
    return (tendency, gradient.transpose(1, 0, 2))


def solution(mesh):
    in_specs = (
        P(ALL, None, None),
        P(ALL, None),
        P(ALL, None),
        P(None, ALL),
        P(ALL),
        P(None, ALL),
        P(ALL),
        P(None, ALL),
        P(None, ALL),
        P(ALL),
        P(None, None, "lon", None),
        P(None, None, "lon", None),
    )
    out_specs = (P(ALL, None), P(ALL, None, None))
    return jax.shard_map(local, mesh=mesh, in_specs=in_specs, out_specs=out_specs, check_vma=False)
```

```python
import jax
import jax.numpy as jnp
from jax import lax
from jax.experimental import pallas as pl
from jax.experimental.pallas import tpu as pltpu
from jax.sharding import PartitionSpec as P


ALL = ("lat", "lon")
F32 = jnp.float32
BF16 = jnp.bfloat16
MIB = 1 << 20


def call(kernel, out, flops, limit, scratch=(), specs=None):
    extra = {} if specs is None else {"in_specs": specs}
    return pl.pallas_call(
        kernel,
        out_shape=out,
        **extra,
        scratch_shapes=scratch,
        compiler_params=pltpu.CompilerParams(vmem_limit_bytes=limit * MIB),
        cost_estimate=pl.CostEstimate(flops=flops, bytes_accessed=4 * MIB, transcendentals=0),
    )


def pick_kernel(perm_ref, planes_ref, last_ref, out_ref):
    total = perm_ref.shape[1]
    rows = 1024
    data = jnp.concatenate([planes_ref[v] for v in range(planes_ref.shape[0])] + [last_ref[...]], axis=1)

    def block(i, carry):
        start = pl.multiple_of(i * rows, rows)
        index = jnp.transpose(jnp.broadcast_to(perm_ref[:, pl.ds(start, rows)], (128, rows)))
        lanes = lax.broadcasted_iota(jnp.int32, (rows, total), 1)
        hot = (jnp.concatenate([index] * (total // 128), axis=1) == lanes).astype(F32).astype(BF16)
        out_ref[pl.ds(start, rows), :] = jnp.dot(hot, data, preferred_element_type=F32).astype(BF16)
        return carry

    lax.fori_loop(0, total // rows, block, 0)


def pick(perm, planes, last):
    total = perm.shape[1]
    width = (planes.shape[0] + 1) * 128
    out = jax.ShapeDtypeStruct((total, width), BF16)
    return call(pick_kernel, out, 2 * total * total * width, 20)(perm, planes, last)


def restore_kernel(perm_ref, data_ref, planes_ref, last_ref):
    total = perm_ref.shape[1]
    rows = 1024
    planes = planes_ref.shape[0]

    def block(i, carry):
        start = pl.multiple_of(i * rows, rows)
        targets = lax.broadcasted_iota(jnp.int32, (rows, total), 0) + start
        hot = (jnp.broadcast_to(perm_ref[...], (rows, total)) == targets).astype(F32).astype(BF16)
        got = jnp.dot(hot, data_ref[...], preferred_element_type=F32).astype(BF16)
        for v in range(planes):
            planes_ref[v, pl.ds(start, rows), :] = got[:, v * 128 : (v + 1) * 128]
        last_ref[pl.ds(start, rows), :] = got[:, planes * 128 :]
        return carry

    lax.fori_loop(0, total // rows, block, 0)


def restore(perm, data):
    total, width = data.shape
    planes = width // 128 - 1
    out = [
        jax.ShapeDtypeStruct((planes, total, 128), BF16),
        jax.ShapeDtypeStruct((total, 128), BF16),
    ]
    return call(restore_kernel, out, 2 * total * total * width, 20)(perm, data)


def two_hot(index_ref, share_ref, out_ref):
    rows, count = out_ref.shape
    block = 256
    first, second, share = index_ref[0:1, :], index_ref[1:2, :], share_ref[...]
    high = jnp.where(first == second, 1.0, share).astype(BF16)
    low = (1.0 - share).astype(BF16)
    targets = lax.broadcasted_iota(jnp.int32, (block, count), 0).astype(F32).astype(BF16)
    spread = lambda row: jnp.broadcast_to(row, (block, count))

    def step(i, carry):
        start = pl.multiple_of(i * block, block)
        one = spread((first - start).astype(F32).astype(BF16)) == targets
        two = spread((second - start).astype(F32).astype(BF16)) == targets
        out_ref[pl.ds(start, block), :] = jnp.where(
            one, spread(high), jnp.where(two, spread(low), jnp.zeros((), BF16))
        )
        return carry

    lax.fori_loop(0, rows // block, step, 0)


def radiation_kernel(
    data_ref,
    bidx_ref,
    bw_ref,
    cidx_ref,
    cw_ref,
    scale_ref,
    ta_hbm,
    tb_hbm,
    out_ref,
    ta_ref,
    tb_ref,
    sems,
    back_ref,
    coarse_ref,
    tt_ref,
    rows_ref,
    adj_ref,
    mid_ref,
    heat_ref,
):
    bands, width, _ = ta_ref.shape
    cols, _ = coarse_ref.shape
    half = 1024

    loads = [
        pltpu.make_async_copy(ta_hbm, ta_ref, sems.at[0]),
        pltpu.make_async_copy(tb_hbm, tb_ref, sems.at[1]),
    ]
    for load in loads:
        load.start()
    two_hot(bidx_ref, bw_ref, back_ref)
    two_hot(cidx_ref, cw_ref, coarse_ref)

    def adjoint(carry):
        adj_ref[...] = jnp.dot(back_ref[...], data_ref[:, width:], preferred_element_type=F32).T
        return carry

    def lift(carry):
        tables = [ref[b] for ref in (ta_ref, tb_ref) for b in range(bands)]
        lifted = jnp.concatenate(
            [(adj_ref[...] * scale_ref[b : b + 1, :]).astype(BF16) for b in range(2 * bands)], axis=0
        )
        got = jnp.dot(jnp.concatenate(tables, axis=1), lifted, preferred_element_type=F32)
        rows_ref[...] = got.T.astype(BF16)
        return carry

    def scatter(i, carry):
        start = pl.multiple_of(i * half, half)
        out_ref[pl.ds(start, half), :width] = jnp.dot(
            coarse_ref[pl.ds(start, half), :], rows_ref[...], preferred_element_type=F32
        ).astype(BF16)
        return carry

    def interpolate(carry):
        mid_ref[...] = lax.dot_general(
            data_ref[:, :width], coarse_ref[...], (((0,), (0,)), ((), ())), preferred_element_type=F32
        ).astype(BF16)
        return carry

    def heat(carry):
        lifted = jnp.concatenate(
            [
                mid_ref[...] * jnp.broadcast_to(scale_ref[b : b + 1, :].astype(BF16), mid_ref.shape)
                for b in range(2 * bands)
            ],
            axis=0,
        )
        heat_ref[...] = jnp.dot(tt_ref[...], lifted, preferred_element_type=F32).astype(BF16)
        return carry

    def back(carry):
        tendency = jnp.dot(heat_ref[...], back_ref[...], preferred_element_type=F32)
        out_ref[:, width:] = tendency.T.astype(BF16)
        return carry

    adjoint(0)
    for load in loads:
        load.wait()
    lift(0)
    lax.fori_loop(0, cols // half, scatter, 0)
    interpolate(0)
    for part, ref in enumerate((ta_ref, tb_ref)):
        for b in range(bands):
            at = (part * bands + b) * width
            tt_ref[:, at : at + width] = ref[b].T
    heat(0)
    back(0)


def radiation(data, bidx, bw, cidx, cw, scale, ta, tb):
    cols, rows = bw.shape[1], cw.shape[1]
    bands, width, levels = ta.shape
    out = jax.ShapeDtypeStruct((cols, width + levels), BF16)
    flops = 8 * bands * rows * levels * width
    scratch = [
        pltpu.VMEM(ta.shape, BF16),
        pltpu.VMEM(tb.shape, BF16),
        pltpu.SemaphoreType.DMA((2,)),
        pltpu.VMEM((rows, cols), BF16),
        pltpu.VMEM((cols, rows), BF16),
        pltpu.VMEM((levels, 2 * bands * width), BF16),
        pltpu.VMEM((rows, width), BF16),
        pltpu.VMEM((levels, rows), F32),
        pltpu.VMEM((width, rows), BF16),
        pltpu.VMEM((levels, rows), BF16),
    ]
    near, far = pl.BlockSpec(memory_space=pltpu.VMEM), pl.BlockSpec(memory_space=pl.ANY)
    specs = [near] * 6 + [far] * 2
    kernel = call(radiation_kernel, out, flops, 34, scratch, specs)
    return kernel(data, bidx, bw, cidx, cw, scale, ta, tb)


def gather_four(block, stride):
    lon = lax.axis_size("lon")
    place = lax.rem(lax.axis_index("lon") // stride, 4)
    size = block.shape[0]
    out = jnp.zeros((4 * size,) + block.shape[1:], block.dtype)
    got = [block]
    for shift in (1, 3, 2):
        pairs = []
        for a in range(lon):
            at = a // stride % 4
            pairs.append((a, a + ((at + shift) % 4 - at) * stride))
        got.append(lax.ppermute(block, "lon", pairs))
    for shift, piece in zip((0, 1, 3, 2), got):
        out = lax.dynamic_update_slice_in_dim(
            out, piece, lax.rem(place + 4 - shift, 4) * size, axis=0
        )
    return out


def exchange(values, axes):
    return lax.all_to_all(values, axes, split_axis=0, concat_axis=0, tiled=True)


def local(
    increments,
    cotangent,
    owner_perm,
    coarse_index,
    coarse_weight,
    back_index,
    back_weight,
    lw_scale,
    sw_scale,
    sunlit,
    lw_table,
    sw_table,
):
    lat = lax.axis_size("lat")
    core = lax.rem(lax.axis_index("lat"), 2)
    table = jnp.concatenate([lw_table, sw_table], axis=0)
    bands, _, _, levels = table.shape
    half = bands // 2
    mine = lax.dynamic_slice_in_dim(table, core * half, half, axis=0)
    column = gather_four(mine[None], 1)
    whole = gather_four(column, 4)
    partner = [(a, a + 1 - 2 * (a % 2)) for a in range(lat)]
    other = lax.ppermute(whole, "lat", partner)
    mine, other = (
        t.transpose(1, 2, 0, 3, 4).reshape(half, -1, levels) for t in (whole, other)
    )
    scale = jnp.concatenate([lw_scale, sw_scale * sunlit.astype(F32)[None, :]], axis=0)
    scale = jnp.where(core == 0, scale, jnp.roll(scale, half, axis=0))
    scale = jnp.pad(scale, ((0, 2), (0, 0)))

    cw = coarse_weight[None]
    bw = back_weight[None]
    planes = increments.transpose(1, 0, 2)
    data = pick(owner_perm, planes, cotangent)
    data = exchange(data, ALL)
    back = radiation(data, back_index, bw, coarse_index, cw, scale, mine, other)
    back = exchange(back, ALL)
    gradient, tendency = restore(owner_perm, back)
    return (tendency, gradient.transpose(1, 0, 2))


def solution(mesh):
    in_specs = (
        P(ALL, None, None),
        P(ALL, None),
        P(ALL, None),
        P(None, ALL),
        P(ALL),
        P(None, ALL),
        P(ALL),
        P(None, ALL),
        P(None, ALL),
        P(ALL),
        P(None, None, "lon", None),
        P(None, None, "lon", None),
    )
    out_specs = (P(ALL, None), P(ALL, None, None))
    return jax.shard_map(local, mesh=mesh, in_specs=in_specs, out_specs=out_specs, check_vma=False)
```

```python
import jax
import jax.numpy as jnp
from jax import lax
from jax.experimental import pallas as pl
from jax.experimental.pallas import tpu as pltpu
from jax.sharding import PartitionSpec as P


ALL = ("lat", "lon")
F32 = jnp.float32
BF16 = jnp.bfloat16
MIB = 1 << 20


def call(kernel, out, flops, limit, scratch=(), specs=None, out_specs=None):
    extra = {} if specs is None else {"in_specs": specs}
    if out_specs is not None:
        extra["out_specs"] = out_specs
    return pl.pallas_call(
        kernel,
        out_shape=out,
        **extra,
        scratch_shapes=scratch,
        compiler_params=pltpu.CompilerParams(vmem_limit_bytes=limit * MIB),
        cost_estimate=pl.CostEstimate(flops=flops, bytes_accessed=4 * MIB, transcendentals=0),
    )


PICK_BLOCKS = (512, 512, 512, 512)


def starts(blocks):
    return [sum(blocks[:k]) for k in range(len(blocks))]


def pick_kernel(perm_hbm, planes_hbm, last_hbm, out_hbm, perm_ref, data_ref, hot_ref, out_ref, in_sems, out_sems):
    total = perm_ref.shape[1]
    planes = planes_hbm.shape[0]
    first = pltpu.make_async_copy(perm_hbm, perm_ref, in_sems.at[planes + 1])
    first.start()
    loads = [pltpu.make_async_copy(planes_hbm.at[v], data_ref.at[v], in_sems.at[v]) for v in range(planes)]
    loads.append(pltpu.make_async_copy(last_hbm, data_ref.at[planes], in_sems.at[planes]))
    for load in loads:
        load.start()
    first.wait()

    def fill(k):
        start, rows = starts(PICK_BLOCKS)[k], PICK_BLOCKS[k]
        index = jnp.transpose(jnp.broadcast_to(perm_ref[:, start : start + rows], (128, rows)))
        lanes = lax.broadcasted_iota(jnp.int32, (rows, total), 1)
        hot = jnp.concatenate([index] * (total // 128), axis=1) == lanes
        hot_ref[k % 2, :rows, :] = hot.astype(F32).astype(BF16)

    fill(0)
    for load in loads:
        load.wait()
    stores = []
    for k, (start, rows) in enumerate(zip(starts(PICK_BLOCKS), PICK_BLOCKS)):
        data = jnp.concatenate([data_ref[v] for v in range(planes + 1)], axis=1)
        got = jnp.dot(hot_ref[k % 2, :rows, :], data, preferred_element_type=F32)
        out_ref[start : start + rows, :] = got.astype(BF16)
        stores.append(
            pltpu.make_async_copy(
                out_ref.at[pl.ds(start, rows), :], out_hbm.at[pl.ds(start, rows), :], out_sems.at[k]
            )
        )
        stores[-1].start()
        if k + 1 < len(PICK_BLOCKS):
            fill(k + 1)
    for store in stores:
        store.wait()


def pick(perm, planes, last):
    total = perm.shape[1]
    count = planes.shape[0] + 1
    out = jax.ShapeDtypeStruct((total, count * 128), BF16)
    far = pl.BlockSpec(memory_space=pl.ANY)
    scratch = [
        pltpu.VMEM(perm.shape, jnp.int32),
        pltpu.VMEM((count, total, 128), BF16),
        pltpu.VMEM((2, max(PICK_BLOCKS), total), BF16),
        pltpu.VMEM((total, count * 128), BF16),
        pltpu.SemaphoreType.DMA((count + 1,)),
        pltpu.SemaphoreType.DMA((len(PICK_BLOCKS),)),
    ]
    flops = 2 * total * total * count * 128
    return call(pick_kernel, out, flops, 60, scratch, [far] * 3, far)(perm, planes, last)


RESTORE_BLOCKS = (1024, 512, 512)


def restore_kernel(perm_ref, data_ref, planes_hbm, last_hbm, hot_ref, out_ref, sems):
    total = perm_ref.shape[1]
    planes = planes_hbm.shape[0]

    def fill(k):
        start, rows = starts(RESTORE_BLOCKS)[k], RESTORE_BLOCKS[k]
        targets = lax.broadcasted_iota(jnp.int32, (rows, total), 0) + start
        hot = jnp.broadcast_to(perm_ref[...], (rows, total)) == targets
        hot_ref[k % 2, :rows, :] = hot.astype(F32).astype(BF16)

    fill(0)
    stores = []
    for k, (start, rows) in enumerate(zip(starts(RESTORE_BLOCKS), RESTORE_BLOCKS)):
        got = jnp.dot(hot_ref[k % 2, :rows, :], data_ref[...], preferred_element_type=F32).astype(BF16)
        for v in range(planes + 1):
            out_ref[v, start : start + rows, :] = got[:, v * 128 : (v + 1) * 128]
        span = pl.ds(start, rows)
        stores.append(
            pltpu.make_async_copy(
                out_ref.at[pl.ds(0, planes), span, :], planes_hbm.at[:, span, :], sems.at[k, 0]
            )
        )
        stores.append(pltpu.make_async_copy(out_ref.at[planes, span, :], last_hbm.at[span, :], sems.at[k, 1]))
        stores[-2].start()
        stores[-1].start()
        if k + 1 < len(RESTORE_BLOCKS):
            fill(k + 1)
    for store in stores:
        store.wait()


def restore(perm, data):
    total, width = data.shape
    planes = width // 128 - 1
    out = [
        jax.ShapeDtypeStruct((planes, total, 128), BF16),
        jax.ShapeDtypeStruct((total, 128), BF16),
    ]
    near, far = pl.BlockSpec(memory_space=pltpu.VMEM), pl.BlockSpec(memory_space=pl.ANY)
    scratch = [
        pltpu.VMEM((2, max(RESTORE_BLOCKS), total), BF16),
        pltpu.VMEM((planes + 1, total, 128), BF16),
        pltpu.SemaphoreType.DMA((len(RESTORE_BLOCKS), 2)),
    ]
    flops = 2 * total * total * width
    return call(restore_kernel, out, flops, 40, scratch, [near] * 2, [far] * 2)(perm, data)


def two_hot(index_ref, share_ref, out_ref):
    rows, count = out_ref.shape
    block = 256
    first, second, share = index_ref[0:1, :], index_ref[1:2, :], share_ref[...]
    high = jnp.where(first == second, 1.0, share).astype(BF16)
    low = (1.0 - share).astype(BF16)
    targets = lax.broadcasted_iota(jnp.int32, (block, count), 0).astype(F32).astype(BF16)
    spread = lambda row: jnp.broadcast_to(row, (block, count))

    def step(i, carry):
        start = pl.multiple_of(i * block, block)
        one = spread((first - start).astype(F32).astype(BF16)) == targets
        two = spread((second - start).astype(F32).astype(BF16)) == targets
        out_ref[pl.ds(start, block), :] = jnp.where(
            one, spread(high), jnp.where(two, spread(low), jnp.zeros((), BF16))
        )
        return carry

    lax.fori_loop(0, rows // block, step, 0)


def radiation_kernel(
    data_ref,
    bidx_ref,
    bw_ref,
    cidx_ref,
    cw_ref,
    scale_ref,
    ta_hbm,
    tb_hbm,
    out_ref,
    ta_ref,
    tb_ref,
    sems,
    back_ref,
    coarse_ref,
    tt_ref,
    rows_ref,
    adj_ref,
    mid_ref,
    heat_ref,
):
    bands, width, _ = ta_ref.shape
    cols, rows = coarse_ref.shape

    loads = [
        pltpu.make_async_copy(ta_hbm, ta_ref, sems.at[0]),
        pltpu.make_async_copy(tb_hbm, tb_ref, sems.at[1]),
    ]
    for load in loads:
        load.start()
    two_hot(bidx_ref, bw_ref, back_ref)
    two_hot(cidx_ref, cw_ref, coarse_ref)

    def adjoint(i, carry):
        s = pl.multiple_of(i * 512, 512)
        adj_ref[:, pl.ds(s, 512)] = jnp.dot(back_ref[pl.ds(s, 512), :], data_ref[:, width:], preferred_element_type=F32).T
        return carry

    def lift(i, carry):
        s = pl.multiple_of(i * 1024, 1024)
        tables = [ref[b] for ref in (ta_ref, tb_ref) for b in range(bands)]
        adj = adj_ref[:, pl.ds(s, 1024)]
        lifted = jnp.concatenate(
            [(adj * scale_ref[b : b + 1, pl.ds(s, 1024)]).astype(BF16) for b in range(2 * bands)], axis=0
        )
        got = jnp.dot(jnp.concatenate(tables, axis=1), lifted, preferred_element_type=F32)
        rows_ref[pl.ds(s, 1024), :] = got.T.astype(BF16)
        return carry

    def scatter(i, carry):
        start = pl.multiple_of(i * 1024, 1024)
        out_ref[pl.ds(start, 1024), :width] = jnp.dot(
            coarse_ref[pl.ds(start, 1024), :], rows_ref[...], preferred_element_type=F32
        ).astype(BF16)
        return carry

    def interpolate(i, carry):
        s = pl.multiple_of(i * 1024, 1024)
        mid_ref[:, pl.ds(s, 1024)] = lax.dot_general(
            data_ref[:, :width], coarse_ref[:, pl.ds(s, 1024)], (((0,), (0,)), ((), ())), preferred_element_type=F32
        ).astype(BF16)
        return carry

    def heat(i, carry):
        s = pl.multiple_of(i * 1024, 1024)
        mid = mid_ref[:, pl.ds(s, 1024)]
        lifted = jnp.concatenate(
            [
                mid * jnp.broadcast_to(scale_ref[b : b + 1, pl.ds(s, 1024)].astype(BF16), mid.shape)
                for b in range(2 * bands)
            ],
            axis=0,
        )
        heat_ref[:, pl.ds(s, 1024)] = jnp.dot(tt_ref[...], lifted, preferred_element_type=F32).astype(BF16)
        return carry

    def back(i, carry):
        s = pl.multiple_of(i * 2048, 2048)
        tendency = jnp.dot(heat_ref[...], back_ref[:, pl.ds(s, 2048)], preferred_element_type=F32)
        out_ref[pl.ds(s, 2048), width:] = tendency.T.astype(BF16)
        return carry

    lax.fori_loop(0, rows // 512, adjoint, 0)
    for load in loads:
        load.wait()
    lax.fori_loop(0, rows // 1024, lift, 0)
    lax.fori_loop(0, cols // 1024, scatter, 0)
    lax.fori_loop(0, rows // 1024, interpolate, 0)
    for part, ref in enumerate((ta_ref, tb_ref)):
        for b in range(bands):
            at = (part * bands + b) * width
            tt_ref[:, at : at + width] = ref[b].T
    lax.fori_loop(0, rows // 1024, heat, 0)
    lax.fori_loop(0, cols // 2048, back, 0)


def radiation(data, bidx, bw, cidx, cw, scale, ta, tb):
    cols, rows = bw.shape[1], cw.shape[1]
    bands, width, levels = ta.shape
    out = jax.ShapeDtypeStruct((cols, width + levels), BF16)
    flops = 8 * bands * rows * levels * width
    scratch = [
        pltpu.VMEM(ta.shape, BF16),
        pltpu.VMEM(tb.shape, BF16),
        pltpu.SemaphoreType.DMA((2,)),
        pltpu.VMEM((rows, cols), BF16),
        pltpu.VMEM((cols, rows), BF16),
        pltpu.VMEM((levels, 2 * bands * width), BF16),
        pltpu.VMEM((rows, width), BF16),
        pltpu.VMEM((levels, rows), F32),
        pltpu.VMEM((width, rows), BF16),
        pltpu.VMEM((levels, rows), BF16),
    ]
    near, far = pl.BlockSpec(memory_space=pltpu.VMEM), pl.BlockSpec(memory_space=pl.ANY)
    specs = [near] * 6 + [far] * 2
    kernel = call(radiation_kernel, out, flops, 34, scratch, specs)
    return kernel(data, bidx, bw, cidx, cw, scale, ta, tb)


def gather_four(block, stride):
    lon = lax.axis_size("lon")
    place = lax.rem(lax.axis_index("lon") // stride, 4)
    size = block.shape[0]
    out = jnp.zeros((4 * size,) + block.shape[1:], block.dtype)
    got = [block]
    for shift in (1, 3, 2):
        pairs = []
        for a in range(lon):
            at = a // stride % 4
            pairs.append((a, a + ((at + shift) % 4 - at) * stride))
        got.append(lax.ppermute(block, "lon", pairs))
    for shift, piece in zip((0, 1, 3, 2), got):
        out = lax.dynamic_update_slice_in_dim(
            out, piece, lax.rem(place + 4 - shift, 4) * size, axis=0
        )
    return out


def exchange(values, axes):
    return lax.all_to_all(values, axes, split_axis=0, concat_axis=0, tiled=True)


def local(
    increments,
    cotangent,
    owner_perm,
    coarse_index,
    coarse_weight,
    back_index,
    back_weight,
    lw_scale,
    sw_scale,
    sunlit,
    lw_table,
    sw_table,
):
    lat = lax.axis_size("lat")
    core = lax.rem(lax.axis_index("lat"), 2)
    table = jnp.concatenate([lw_table, sw_table], axis=0)
    bands, _, _, levels = table.shape
    half = bands // 2
    mine = lax.dynamic_slice_in_dim(table, core * half, half, axis=0)
    column = gather_four(mine[None], 1)
    whole = gather_four(column, 4)
    partner = [(a, a + 1 - 2 * (a % 2)) for a in range(lat)]
    other = lax.ppermute(whole, "lat", partner)
    mine, other = (
        t.transpose(1, 2, 0, 3, 4).reshape(half, -1, levels) for t in (whole, other)
    )
    scale = jnp.concatenate([lw_scale, sw_scale * sunlit.astype(F32)[None, :]], axis=0)
    scale = jnp.where(core == 0, scale, jnp.roll(scale, half, axis=0))
    scale = jnp.pad(scale, ((0, 2), (0, 0)))

    cw = coarse_weight[None]
    bw = back_weight[None]
    planes = increments.transpose(1, 0, 2)
    data = pick(owner_perm, planes, cotangent)
    data = exchange(data, ALL)
    back = radiation(data, back_index, bw, coarse_index, cw, scale, mine, other)
    back = exchange(back, ALL)
    gradient, tendency = restore(owner_perm, back)
    return (tendency, gradient.transpose(1, 0, 2))


def solution(mesh):
    in_specs = (
        P(ALL, None, None),
        P(ALL, None),
        P(ALL, None),
        P(None, ALL),
        P(ALL),
        P(None, ALL),
        P(ALL),
        P(None, ALL),
        P(None, ALL),
        P(ALL),
        P(None, None, "lon", None),
        P(None, None, "lon", None),
    )
    out_specs = (P(ALL, None), P(ALL, None, None))
    return jax.shard_map(local, mesh=mesh, in_specs=in_specs, out_specs=out_specs, check_vma=False)
```

```python
import jax
import jax.numpy as jnp
from jax import lax
from jax.experimental import pallas as pl
from jax.experimental.pallas import tpu as pltpu
from jax.sharding import PartitionSpec as P


ALL = ("lat", "lon")
F32 = jnp.float32
BF16 = jnp.bfloat16
MIB = 1 << 20


def call(kernel, out, flops, limit, scratch=(), specs=None, out_specs=None, aliases=None):
    extra = {} if specs is None else {"in_specs": specs}
    if out_specs is not None:
        extra["out_specs"] = out_specs
    if aliases is not None:
        extra["input_output_aliases"] = aliases
    return pl.pallas_call(
        kernel,
        out_shape=out,
        **extra,
        scratch_shapes=scratch,
        compiler_params=pltpu.CompilerParams(vmem_limit_bytes=limit * MIB),
        cost_estimate=pl.CostEstimate(flops=flops, bytes_accessed=4 * MIB, transcendentals=0),
    )


PICK_BLOCKS = (512, 512, 512, 512)


def starts(blocks):
    return [sum(blocks[:k]) for k in range(len(blocks))]


def pick_kernel(perm_hbm, planes_hbm, out_hbm, perm_ref, data_ref, hot_ref, out_ref, in_sems, out_sems):
    total = perm_ref.shape[1]
    planes = planes_hbm.shape[0]
    first = pltpu.make_async_copy(perm_hbm, perm_ref, in_sems.at[planes])
    first.start()
    loads = [pltpu.make_async_copy(planes_hbm.at[v], data_ref.at[v], in_sems.at[v]) for v in range(planes)]
    for load in loads:
        load.start()
    first.wait()

    def fill(k):
        start, rows = starts(PICK_BLOCKS)[k], PICK_BLOCKS[k]
        index = jnp.transpose(jnp.broadcast_to(perm_ref[:, start : start + rows], (128, rows)))
        lanes = lax.broadcasted_iota(jnp.int32, (rows, total), 1)
        hot = jnp.concatenate([index] * (total // 128), axis=1) == lanes
        hot_ref[k % 2, :rows, :] = hot.astype(F32).astype(BF16)

    fill(0)
    for load in loads:
        load.wait()
    stores = []
    for k, (start, rows) in enumerate(zip(starts(PICK_BLOCKS), PICK_BLOCKS)):
        data = jnp.concatenate([data_ref[v] for v in range(planes)], axis=1)
        got = jnp.dot(hot_ref[k % 2, :rows, :], data, preferred_element_type=F32)
        out_ref[start : start + rows, :] = got.astype(BF16)
        stores.append(
            pltpu.make_async_copy(
                out_ref.at[pl.ds(start, rows), :], out_hbm.at[pl.ds(start, rows), :], out_sems.at[k]
            )
        )
        stores[-1].start()
        if k + 1 < len(PICK_BLOCKS):
            fill(k + 1)
    for store in stores:
        store.wait()


def pick(perm, planes):
    total = perm.shape[1]
    count = planes.shape[0]
    out = jax.ShapeDtypeStruct((total, count * 128), BF16)
    far = pl.BlockSpec(memory_space=pl.ANY)
    scratch = [
        pltpu.VMEM(perm.shape, jnp.int32),
        pltpu.VMEM((count, total, 128), BF16),
        pltpu.VMEM((2, max(PICK_BLOCKS), total), BF16),
        pltpu.VMEM((total, count * 128), BF16),
        pltpu.SemaphoreType.DMA((count + 1,)),
        pltpu.SemaphoreType.DMA((len(PICK_BLOCKS),)),
    ]
    flops = 2 * total * total * count * 128
    return call(pick_kernel, out, flops, 60, scratch, [far] * 2, far)(perm, planes)


RESTORE_BLOCKS = (1024, 512, 512)


def restore_kernel(perm_ref, data_ref, planes_hbm, last_hbm, hot_ref, out_ref, sems):
    total = perm_ref.shape[1]
    planes = planes_hbm.shape[0]

    def fill(k):
        start, rows = starts(RESTORE_BLOCKS)[k], RESTORE_BLOCKS[k]
        targets = lax.broadcasted_iota(jnp.int32, (rows, total), 0) + start
        hot = jnp.broadcast_to(perm_ref[...], (rows, total)) == targets
        hot_ref[k % 2, :rows, :] = hot.astype(F32).astype(BF16)

    fill(0)
    stores = []
    for k, (start, rows) in enumerate(zip(starts(RESTORE_BLOCKS), RESTORE_BLOCKS)):
        got = jnp.dot(hot_ref[k % 2, :rows, :], data_ref[...], preferred_element_type=F32).astype(BF16)
        for v in range(planes + 1):
            out_ref[v, start : start + rows, :] = got[:, v * 128 : (v + 1) * 128]
        span = pl.ds(start, rows)
        stores.append(
            pltpu.make_async_copy(
                out_ref.at[pl.ds(0, planes), span, :], planes_hbm.at[:, span, :], sems.at[k, 0]
            )
        )
        stores.append(pltpu.make_async_copy(out_ref.at[planes, span, :], last_hbm.at[span, :], sems.at[k, 1]))
        stores[-2].start()
        stores[-1].start()
        if k + 1 < len(RESTORE_BLOCKS):
            fill(k + 1)
    for store in stores:
        store.wait()


def restore(perm, data):
    total, width = data.shape
    planes = width // 128 - 1
    out = [
        jax.ShapeDtypeStruct((planes, total, 128), BF16),
        jax.ShapeDtypeStruct((total, 128), BF16),
    ]
    near, far = pl.BlockSpec(memory_space=pltpu.VMEM), pl.BlockSpec(memory_space=pl.ANY)
    scratch = [
        pltpu.VMEM((2, max(RESTORE_BLOCKS), total), BF16),
        pltpu.VMEM((planes + 1, total, 128), BF16),
        pltpu.SemaphoreType.DMA((len(RESTORE_BLOCKS), 2)),
    ]
    flops = 2 * total * total * width
    return call(restore_kernel, out, flops, 40, scratch, [near] * 2, [far] * 2)(perm, data)


def two_hot(index_ref, share_ref, out_ref):
    rows, count = out_ref.shape
    block = 256
    first, second, share = index_ref[0:1, :], index_ref[1:2, :], share_ref[...]
    high = jnp.where(first == second, 1.0, share).astype(BF16)
    low = (1.0 - share).astype(BF16)
    targets = lax.broadcasted_iota(jnp.int32, (block, count), 0).astype(F32).astype(BF16)
    spread = lambda row: jnp.broadcast_to(row, (block, count))

    def step(i, carry):
        start = pl.multiple_of(i * block, block)
        one = spread((first - start).astype(F32).astype(BF16)) == targets
        two = spread((second - start).astype(F32).astype(BF16)) == targets
        out_ref[pl.ds(start, block), :] = jnp.where(
            one, spread(high), jnp.where(two, spread(low), jnp.zeros((), BF16))
        )
        return carry

    lax.fori_loop(0, rows // block, step, 0)


def adjoint_kernel(
    cot_ref,
    bidx_ref,
    bw_ref,
    cidx_ref,
    cw_ref,
    scale_ref,
    ta_hbm,
    tb_hbm,
    out_hbm,
    back_hbm,
    tt_hbm,
    ta_ref,
    tb_ref,
    back_ref,
    coarse_ref,
    tt_ref,
    rows_ref,
    adj_ref,
    grad_ref,
    sems,
):
    bands, width, _ = ta_ref.shape
    cols, rows = coarse_ref.shape
    loads = [
        pltpu.make_async_copy(ta_hbm, ta_ref, sems.at[0]),
        pltpu.make_async_copy(tb_hbm, tb_ref, sems.at[1]),
    ]
    for load in loads:
        load.start()
    two_hot(bidx_ref, bw_ref, back_ref)
    store_back = pltpu.make_async_copy(back_ref, back_hbm, sems.at[2])
    store_back.start()
    two_hot(cidx_ref, cw_ref, coarse_ref)

    def adjoint(i, carry):
        s = pl.multiple_of(i * 512, 512)
        adj_ref[:, pl.ds(s, 512)] = jnp.dot(
            back_ref[pl.ds(s, 512), :], cot_ref[...], preferred_element_type=F32
        ).T
        return carry

    lax.fori_loop(0, rows // 512, adjoint, 0)
    for load in loads:
        load.wait()
    for part, ref in enumerate((ta_ref, tb_ref)):
        for b in range(bands):
            at = (part * bands + b) * width
            tt_ref[:, at : at + width] = ref[b].T
    store_turned = pltpu.make_async_copy(tt_ref, tt_hbm, sems.at[3])
    store_turned.start()
    tables = [ref[b] for ref in (ta_ref, tb_ref) for b in range(bands)]
    lifted = jnp.concatenate(
        [(adj_ref[...] * scale_ref[b : b + 1, :]).astype(BF16) for b in range(2 * bands)], axis=0
    )
    rows_ref[...] = jnp.dot(
        jnp.concatenate(tables, axis=1), lifted, preferred_element_type=F32
    ).astype(BF16)

    def scatter(i, carry):
        s = pl.multiple_of(i * 1024, 1024)
        got = lax.dot_general(
            rows_ref[...],
            coarse_ref[pl.ds(s, 1024), :],
            (((1,), (1,)), ((), ())),
            preferred_element_type=F32,
        )
        grad_ref[pl.ds(s, 1024), :] = got.T.astype(BF16)
        return carry

    lax.fori_loop(0, cols // 1024, scatter, 0)
    store_grad = pltpu.make_async_copy(grad_ref, out_hbm.at[:, pl.ds(0, width)], sems.at[4])
    store_grad.start()
    for store in (store_back, store_turned, store_grad):
        store.wait()


def adjoint_part(cot, bidx, bw, cidx, cw, scale, ta, tb):
    cols, rows = bw.shape[1], cw.shape[1]
    bands, width, levels = ta.shape
    turned = (levels, 2 * bands * width)
    out = [
        jax.ShapeDtypeStruct((cols, width + levels), BF16),
        jax.ShapeDtypeStruct((rows, cols), BF16),
        jax.ShapeDtypeStruct(turned, BF16),
    ]
    scratch = [
        pltpu.VMEM(ta.shape, BF16),
        pltpu.VMEM(tb.shape, BF16),
        pltpu.VMEM((rows, cols), BF16),
        pltpu.VMEM((cols, rows), BF16),
        pltpu.VMEM(turned, BF16),
        pltpu.VMEM((width, rows), BF16),
        pltpu.VMEM((levels, rows), F32),
        pltpu.VMEM((cols, width), BF16),
        pltpu.SemaphoreType.DMA((5,)),
    ]
    near, far = pl.BlockSpec(memory_space=pltpu.VMEM), pl.BlockSpec(memory_space=pl.ANY)
    flops = 4 * bands * rows * levels * width
    kernel = call(adjoint_kernel, out, flops, 60, scratch, [near] * 6 + [far] * 2, [far] * 3)
    return kernel(cot, bidx, bw, cidx, cw, scale, ta, tb)


def forward_kernel(
    fields_ref,
    cidx_ref,
    cw_ref,
    scale_ref,
    back_hbm,
    tt_hbm,
    whole_hbm,
    out_hbm,
    back_ref,
    coarse_ref,
    tt_ref,
    mid_ref,
    heat_ref,
    tend_ref,
    sems,
):
    del whole_hbm
    width = fields_ref.shape[1]
    rows = coarse_ref.shape[1]
    bands = tt_ref.shape[1] // width
    loads = [
        pltpu.make_async_copy(tt_hbm, tt_ref, sems.at[0]),
        pltpu.make_async_copy(back_hbm, back_ref, sems.at[1]),
    ]
    for load in loads:
        load.start()
    two_hot(cidx_ref, cw_ref, coarse_ref)

    def interpolate(i, carry):
        s = pl.multiple_of(i * 512, 512)
        mid_ref[:, pl.ds(s, 512)] = lax.dot_general(
            fields_ref[...],
            coarse_ref[:, pl.ds(s, 512)],
            (((0,), (0,)), ((), ())),
            preferred_element_type=F32,
        ).astype(BF16)
        return carry

    lax.fori_loop(0, rows // 512, interpolate, 0)
    loads[0].wait()
    lifted = jnp.concatenate(
        [
            mid_ref[...] * jnp.broadcast_to(scale_ref[b : b + 1, :].astype(BF16), mid_ref.shape)
            for b in range(bands)
        ],
        axis=0,
    )
    heat_ref[...] = jnp.dot(tt_ref[...], lifted, preferred_element_type=F32).astype(BF16)
    loads[1].wait()
    tend_ref[...] = jnp.dot(heat_ref[...], back_ref[...], preferred_element_type=F32).T.astype(BF16)
    store = pltpu.make_async_copy(tend_ref, out_hbm.at[:, pl.ds(width, tend_ref.shape[1])], sems.at[2])
    store.start()
    store.wait()


def forward_part(fields, cidx, cw, scale, back, turned, whole):
    cols, width = fields.shape
    rows = cw.shape[1]
    levels = turned.shape[0]
    out = jax.ShapeDtypeStruct(whole.shape, BF16)
    scratch = [
        pltpu.VMEM(back.shape, BF16),
        pltpu.VMEM((cols, rows), BF16),
        pltpu.VMEM(turned.shape, BF16),
        pltpu.VMEM((width, rows), BF16),
        pltpu.VMEM((levels, rows), BF16),
        pltpu.VMEM((cols, levels), BF16),
        pltpu.SemaphoreType.DMA((3,)),
    ]
    near, far = pl.BlockSpec(memory_space=pltpu.VMEM), pl.BlockSpec(memory_space=pl.ANY)
    flops = 2 * turned.shape[1] * rows * levels
    kernel = call(forward_kernel, out, flops, 60, scratch, [near] * 4 + [far] * 3, far, {6: 0})
    return kernel(fields, cidx, cw, scale, back, turned, whole)


def gather_four(block, stride):
    lon = lax.axis_size("lon")
    place = lax.rem(lax.axis_index("lon") // stride, 4)
    size = block.shape[0]
    out = jnp.zeros((4 * size,) + block.shape[1:], block.dtype)
    got = [block]
    for shift in (1, 3, 2):
        pairs = []
        for a in range(lon):
            at = a // stride % 4
            pairs.append((a, a + ((at + shift) % 4 - at) * stride))
        got.append(lax.ppermute(block, "lon", pairs))
    for shift, piece in zip((0, 1, 3, 2), got):
        out = lax.dynamic_update_slice_in_dim(
            out, piece, lax.rem(place + 4 - shift, 4) * size, axis=0
        )
    return out


def exchange(values, axes):
    return lax.all_to_all(values, axes, split_axis=0, concat_axis=0, tiled=True)


def local(
    increments,
    cotangent,
    owner_perm,
    coarse_index,
    coarse_weight,
    back_index,
    back_weight,
    lw_scale,
    sw_scale,
    sunlit,
    lw_table,
    sw_table,
):
    lat = lax.axis_size("lat")
    core = lax.rem(lax.axis_index("lat"), 2)
    table = jnp.concatenate([lw_table, sw_table], axis=0)
    bands, _, _, levels = table.shape
    half = bands // 2
    mine = lax.dynamic_slice_in_dim(table, core * half, half, axis=0)
    column = gather_four(mine[None], 1)
    whole = gather_four(column, 4)
    partner = [(a, a + 1 - 2 * (a % 2)) for a in range(lat)]
    other = lax.ppermute(whole, "lat", partner)
    mine, other = (
        t.transpose(1, 2, 0, 3, 4).reshape(half, -1, levels) for t in (whole, other)
    )
    scale = jnp.concatenate([lw_scale, sw_scale * sunlit.astype(F32)[None, :]], axis=0)
    scale = jnp.where(core == 0, scale, jnp.roll(scale, half, axis=0))
    scale = jnp.pad(scale, ((0, 2), (0, 0)))

    cw = coarse_weight[None]
    bw = back_weight[None]
    sent = pick(owner_perm, cotangent[None])
    cot_rad = exchange(sent, ALL)
    sent = pick(owner_perm, increments.transpose(1, 0, 2))
    fields = exchange(sent, ALL)
    whole, back_weights, turned = adjoint_part(
        cot_rad, back_index, bw, coarse_index, cw, scale, mine, other
    )
    back = forward_part(fields, coarse_index, cw, scale, back_weights, turned, whole)
    back = exchange(back, ALL)
    gradient, tendency = restore(owner_perm, back)
    return (tendency, gradient.transpose(1, 0, 2))


def solution(mesh):
    in_specs = (
        P(ALL, None, None),
        P(ALL, None),
        P(ALL, None),
        P(None, ALL),
        P(ALL),
        P(None, ALL),
        P(ALL),
        P(None, ALL),
        P(None, ALL),
        P(ALL),
        P(None, None, "lon", None),
        P(None, None, "lon", None),
    )
    out_specs = (P(ALL, None), P(ALL, None, None))
    return jax.shard_map(local, mesh=mesh, in_specs=in_specs, out_specs=out_specs, check_vma=False)
```

```python
import jax
import jax.numpy as jnp
from jax import lax
from jax.experimental import pallas as pl
from jax.experimental.pallas import tpu as pltpu
from jax.sharding import PartitionSpec as P


ALL = ("lat", "lon")
F32 = jnp.float32
BF16 = jnp.bfloat16
MIB = 1 << 20


def call(kernel, out, flops, limit, scratch=(), specs=None, out_specs=None):
    extra = {} if specs is None else {"in_specs": specs}
    if out_specs is not None:
        extra["out_specs"] = out_specs
    return pl.pallas_call(
        kernel,
        out_shape=out,
        **extra,
        scratch_shapes=scratch,
        compiler_params=pltpu.CompilerParams(vmem_limit_bytes=limit * MIB),
        cost_estimate=pl.CostEstimate(flops=flops, bytes_accessed=4 * MIB, transcendentals=0),
    )


PICK_BLOCKS = (256, 512, 1024, 256)


def starts(blocks):
    return [sum(blocks[:k]) for k in range(len(blocks))]


def pick_kernel(perm_hbm, planes_hbm, last_hbm, out_hbm, perm_ref, data_ref, hot_ref, out_ref, in_sems, out_sems):
    total = perm_ref.shape[1]
    planes = planes_hbm.shape[0]
    first = pltpu.make_async_copy(perm_hbm, perm_ref, in_sems.at[planes + 1])
    first.start()
    loads = [pltpu.make_async_copy(planes_hbm.at[v], data_ref.at[v], in_sems.at[v]) for v in range(planes)]
    loads.append(pltpu.make_async_copy(last_hbm, data_ref.at[planes], in_sems.at[planes]))
    for load in loads:
        load.start()
    first.wait()

    def fill(k):
        start, rows = starts(PICK_BLOCKS)[k], PICK_BLOCKS[k]
        index = jnp.transpose(jnp.broadcast_to(perm_ref[:, start : start + rows], (128, rows)))
        lanes = lax.broadcasted_iota(jnp.int32, (rows, total), 1)
        hot = jnp.concatenate([index] * (total // 128), axis=1) == lanes
        hot_ref[k % 2, :rows, :] = hot.astype(F32).astype(BF16)

    fill(0)
    for load in loads:
        load.wait()
    stores = []
    for k, (start, rows) in enumerate(zip(starts(PICK_BLOCKS), PICK_BLOCKS)):
        data = jnp.concatenate([data_ref[v] for v in range(planes + 1)], axis=1)
        got = jnp.dot(hot_ref[k % 2, :rows, :], data, preferred_element_type=F32)
        out_ref[start : start + rows, :] = got.astype(BF16)
        stores.append(
            pltpu.make_async_copy(
                out_ref.at[pl.ds(start, rows), :], out_hbm.at[pl.ds(start, rows), :], out_sems.at[k]
            )
        )
        stores[-1].start()
        if k + 1 < len(PICK_BLOCKS):
            fill(k + 1)
    for store in stores:
        store.wait()


def pick(perm, planes, last):
    total = perm.shape[1]
    count = planes.shape[0] + 1
    out = jax.ShapeDtypeStruct((total, count * 128), BF16)
    far = pl.BlockSpec(memory_space=pl.ANY)
    scratch = [
        pltpu.VMEM(perm.shape, jnp.int32),
        pltpu.VMEM((count, total, 128), BF16),
        pltpu.VMEM((2, max(PICK_BLOCKS), total), BF16),
        pltpu.VMEM((total, count * 128), BF16),
        pltpu.SemaphoreType.DMA((count + 1,)),
        pltpu.SemaphoreType.DMA((len(PICK_BLOCKS),)),
    ]
    flops = 2 * total * total * count * 128
    return call(pick_kernel, out, flops, 60, scratch, [far] * 3, far)(perm, planes, last)


RESTORE_BLOCKS = (256, 1024, 512, 256)


def restore_kernel(perm_ref, data_ref, planes_hbm, last_hbm, hot_ref, out_ref, sems):
    total = perm_ref.shape[1]
    planes = planes_hbm.shape[0]

    def fill(k):
        start, rows = starts(RESTORE_BLOCKS)[k], RESTORE_BLOCKS[k]
        targets = lax.broadcasted_iota(jnp.int32, (rows, total), 0) + start
        hot = jnp.broadcast_to(perm_ref[...], (rows, total)) == targets
        hot_ref[k % 2, :rows, :] = hot.astype(F32).astype(BF16)

    fill(0)
    stores = []
    for k, (start, rows) in enumerate(zip(starts(RESTORE_BLOCKS), RESTORE_BLOCKS)):
        got = jnp.dot(hot_ref[k % 2, :rows, :], data_ref[...], preferred_element_type=F32).astype(BF16)
        for v in range(planes + 1):
            out_ref[v, start : start + rows, :] = got[:, v * 128 : (v + 1) * 128]
        span = pl.ds(start, rows)
        stores.append(
            pltpu.make_async_copy(
                out_ref.at[pl.ds(0, planes), span, :], planes_hbm.at[:, span, :], sems.at[k, 0]
            )
        )
        stores.append(pltpu.make_async_copy(out_ref.at[planes, span, :], last_hbm.at[span, :], sems.at[k, 1]))
        stores[-2].start()
        stores[-1].start()
        if k + 1 < len(RESTORE_BLOCKS):
            fill(k + 1)
    for store in stores:
        store.wait()


def restore(perm, data):
    total, width = data.shape
    planes = width // 128 - 1
    out = [
        jax.ShapeDtypeStruct((planes, total, 128), BF16),
        jax.ShapeDtypeStruct((total, 128), BF16),
    ]
    near, far = pl.BlockSpec(memory_space=pltpu.VMEM), pl.BlockSpec(memory_space=pl.ANY)
    scratch = [
        pltpu.VMEM((2, max(RESTORE_BLOCKS), total), BF16),
        pltpu.VMEM((planes + 1, total, 128), BF16),
        pltpu.SemaphoreType.DMA((len(RESTORE_BLOCKS), 2)),
    ]
    flops = 2 * total * total * width
    return call(restore_kernel, out, flops, 40, scratch, [near] * 2, [far] * 2)(perm, data)


ADJOINT_ROWS = 512
SCATTER_ROWS = 1024


def two_hot(index_ref, share_ref, start, rows):
    count = index_ref.shape[1]
    block = 256
    first, second, share = index_ref[0:1, :], index_ref[1:2, :], share_ref[...]
    high = jnp.where(first == second, 1.0, share).astype(BF16)
    low = (1.0 - share).astype(BF16)
    targets = lax.broadcasted_iota(jnp.int32, (block, count), 0).astype(F32).astype(BF16)
    spread = lambda row: jnp.broadcast_to(row, (block, count))
    pieces = []
    for at in range(0, rows, block):
        one = spread((first - (start + at)).astype(F32).astype(BF16)) == targets
        two = spread((second - (start + at)).astype(F32).astype(BF16)) == targets
        pieces.append(jnp.where(one, spread(high), jnp.where(two, spread(low), jnp.zeros((), BF16))))
    return pieces[0] if len(pieces) == 1 else jnp.concatenate(pieces, axis=0)


def radiation_kernel(
    data_ref,
    bidx_ref,
    bw_ref,
    cidx_ref,
    cw_ref,
    scale_ref,
    ta_hbm,
    tb_hbm,
    out_ref,
    table_ref,
    sems,
    back_ref,
    coarse_ref,
    tt_ref,
    rows_ref,
    adj_ref,
    mid_ref,
    heat_ref,
):
    bands, width, _ = table_ref.shape
    cols, rows = coarse_ref.shape
    half = bands // 2
    loads = [
        pltpu.make_async_copy(ta_hbm, table_ref.at[pl.ds(0, half)], sems.at[0]),
        pltpu.make_async_copy(tb_hbm, table_ref.at[pl.ds(half, half)], sems.at[1]),
    ]
    for load in loads:
        load.start()

    def adjoint(i, carry):
        start = pl.multiple_of(i * ADJOINT_ROWS, ADJOINT_ROWS)
        matrix = two_hot(bidx_ref, bw_ref, start, ADJOINT_ROWS)
        back_ref[pl.ds(start, ADJOINT_ROWS), :] = matrix
        adj_ref[:, pl.ds(start, ADJOINT_ROWS)] = jnp.dot(
            matrix, data_ref[:, width:], preferred_element_type=F32
        ).T
        return carry

    lax.fori_loop(0, rows // ADJOINT_ROWS, adjoint, 0)
    for load in loads:
        load.wait()

    lifted = jnp.concatenate(
        [(adj_ref[...] * scale_ref[b : b + 1, :]).astype(BF16) for b in range(bands)], axis=0
    )
    tables = jnp.concatenate([table_ref[b] for b in range(bands)], axis=1)
    rows_ref[...] = jnp.dot(tables, lifted, preferred_element_type=F32).astype(BF16)

    def scatter(i, carry):
        start = pl.multiple_of(i * SCATTER_ROWS, SCATTER_ROWS)
        matrix = two_hot(cidx_ref, cw_ref, start, SCATTER_ROWS)
        coarse_ref[pl.ds(start, SCATTER_ROWS), :] = matrix
        got = lax.dot_general(
            rows_ref[...], matrix, (((1,), (1,)), ((), ())), preferred_element_type=F32
        )
        out_ref[pl.ds(start, SCATTER_ROWS), :width] = got.T.astype(BF16)
        per = bands * SCATTER_ROWS // cols
        for k in range(per):
            b = i * per + k
            tt_ref[:, pl.ds(pl.multiple_of(b * width, 128), width)] = table_ref[b].T
        return carry

    lax.fori_loop(0, cols // SCATTER_ROWS, scatter, 0)

    mid_ref[...] = lax.dot_general(
        data_ref[:, :width], coarse_ref[...], (((0,), (0,)), ((), ())), preferred_element_type=F32
    ).astype(BF16)
    lifted = jnp.concatenate(
        [
            mid_ref[...] * jnp.broadcast_to(scale_ref[b : b + 1, :].astype(BF16), mid_ref.shape)
            for b in range(bands)
        ],
        axis=0,
    )
    heat_ref[...] = jnp.dot(tt_ref[...], lifted, preferred_element_type=F32).astype(BF16)
    tendency = jnp.dot(heat_ref[...], back_ref[...], preferred_element_type=F32)
    out_ref[:, width:] = tendency.T.astype(BF16)


def radiation(data, bidx, bw, cidx, cw, scale, ta, tb):
    cols, rows = bw.shape[1], cw.shape[1]
    bands, width, levels = ta.shape
    out = jax.ShapeDtypeStruct((cols, width + levels), BF16)
    flops = 8 * bands * rows * levels * width
    scratch = [
        pltpu.VMEM((2 * bands, width, levels), BF16),
        pltpu.SemaphoreType.DMA((2,)),
        pltpu.VMEM((rows, cols), BF16),
        pltpu.VMEM((cols, rows), BF16),
        pltpu.VMEM((levels, 2 * bands * width), BF16),
        pltpu.VMEM((width, rows), BF16),
        pltpu.VMEM((levels, rows), F32),
        pltpu.VMEM((width, rows), BF16),
        pltpu.VMEM((levels, rows), BF16),
    ]
    near, far = pl.BlockSpec(memory_space=pltpu.VMEM), pl.BlockSpec(memory_space=pl.ANY)
    specs = [near] * 6 + [far] * 2
    kernel = call(radiation_kernel, out, flops, 34, scratch, specs)
    return kernel(data, bidx, bw, cidx, cw, scale, ta, tb)


def gather_four(block, stride):
    lon = lax.axis_size("lon")
    place = lax.rem(lax.axis_index("lon") // stride, 4)
    size = block.shape[0]
    out = jnp.zeros((4 * size,) + block.shape[1:], block.dtype)
    got = {0: block}
    for shift in (2, 1, 3):
        pairs = []
        for a in range(lon):
            at = a // stride % 4
            pairs.append((a, a + ((at + shift) % 4 - at) * stride))
        got[shift] = lax.ppermute(block, "lon", pairs)
    for shift in (0, 2, 1, 3):
        out = lax.dynamic_update_slice_in_dim(
            out, got[shift], lax.rem(place + 4 - shift, 4) * size, axis=0
        )
    return out


def exchange(values, axes):
    return lax.all_to_all(values, axes, split_axis=0, concat_axis=0, tiled=True)


def local(
    increments,
    cotangent,
    owner_perm,
    coarse_index,
    coarse_weight,
    back_index,
    back_weight,
    lw_scale,
    sw_scale,
    sunlit,
    lw_table,
    sw_table,
):
    lat = lax.axis_size("lat")
    core = lax.rem(lax.axis_index("lat"), 2)
    table = jnp.concatenate([lw_table, sw_table], axis=0)
    bands, _, _, levels = table.shape
    half = bands // 2
    mine = lax.dynamic_slice_in_dim(table, core * half, half, axis=0)
    column = gather_four(mine[None], 1)
    whole = gather_four(column, 4)
    partner = [(a, a + 1 - 2 * (a % 2)) for a in range(lat)]
    other = lax.ppermute(whole, "lat", partner)
    mine, other = (
        t.transpose(1, 2, 0, 3, 4).reshape(half, -1, levels) for t in (whole, other)
    )
    scale = jnp.concatenate([lw_scale, sw_scale * sunlit.astype(F32)[None, :]], axis=0)
    scale = jnp.where(core == 0, scale, jnp.roll(scale, half, axis=0))
    scale = jnp.pad(scale, ((0, 2), (0, 0)))

    cw = coarse_weight[None]
    bw = back_weight[None]
    planes = increments.transpose(1, 0, 2)
    data = pick(owner_perm, planes, cotangent)
    data = exchange(data, ALL)
    back = radiation(data, back_index, bw, coarse_index, cw, scale, mine, other)
    back = exchange(back, ALL)
    gradient, tendency = restore(owner_perm, back)
    return (tendency, gradient.transpose(1, 0, 2))


def solution(mesh):
    in_specs = (
        P(ALL, None, None),
        P(ALL, None),
        P(ALL, None),
        P(None, ALL),
        P(ALL),
        P(None, ALL),
        P(ALL),
        P(None, ALL),
        P(None, ALL),
        P(ALL),
        P(None, None, "lon", None),
        P(None, None, "lon", None),
    )
    out_specs = (P(ALL, None), P(ALL, None, None))
    return jax.shard_map(local, mesh=mesh, in_specs=in_specs, out_specs=out_specs, check_vma=False)
```

```python
import jax
import jax.numpy as jnp
from jax import lax
from jax.experimental import pallas as pl
from jax.experimental.pallas import tpu as pltpu
from jax.sharding import PartitionSpec as P


ALL = ("lat", "lon")
F32 = jnp.float32
BF16 = jnp.bfloat16
MIB = 1 << 20


def call(kernel, out, flops, limit, scratch=(), specs=None, out_specs=None):
    extra = {} if specs is None else {"in_specs": specs}
    if out_specs is not None:
        extra["out_specs"] = out_specs
    return pl.pallas_call(
        kernel,
        out_shape=out,
        **extra,
        scratch_shapes=scratch,
        compiler_params=pltpu.CompilerParams(vmem_limit_bytes=limit * MIB),
        cost_estimate=pl.CostEstimate(flops=flops, bytes_accessed=4 * MIB, transcendentals=0),
    )


PICK_BLOCKS = (256, 512, 1024, 256)


def starts(blocks):
    return [sum(blocks[:k]) for k in range(len(blocks))]


def pick_kernel(perm_hbm, planes_hbm, last_hbm, out_hbm, perm_ref, data_ref, hot_ref, out_ref, in_sems, out_sems):
    total = perm_ref.shape[1]
    planes = planes_hbm.shape[0]
    first = pltpu.make_async_copy(perm_hbm, perm_ref, in_sems.at[planes + 1])
    first.start()
    loads = [pltpu.make_async_copy(planes_hbm.at[v], data_ref.at[v], in_sems.at[v]) for v in range(planes)]
    loads.append(pltpu.make_async_copy(last_hbm, data_ref.at[planes], in_sems.at[planes]))
    for load in loads:
        load.start()
    first.wait()

    def fill(k):
        start, rows = starts(PICK_BLOCKS)[k], PICK_BLOCKS[k]
        index = jnp.transpose(jnp.broadcast_to(perm_ref[:, start : start + rows], (128, rows)))
        lanes = lax.broadcasted_iota(jnp.int32, (rows, total), 1)
        hot = jnp.concatenate([index] * (total // 128), axis=1) == lanes
        hot_ref[k % 2, :rows, :] = hot.astype(F32).astype(BF16)

    fill(0)
    for load in loads:
        load.wait()
    stores = []
    for k, (start, rows) in enumerate(zip(starts(PICK_BLOCKS), PICK_BLOCKS)):
        data = jnp.concatenate([data_ref[v] for v in range(planes + 1)], axis=1)
        got = jnp.dot(hot_ref[k % 2, :rows, :], data, preferred_element_type=F32)
        out_ref[start : start + rows, :] = got.astype(BF16)
        stores.append(
            pltpu.make_async_copy(
                out_ref.at[pl.ds(start, rows), :], out_hbm.at[pl.ds(start, rows), :], out_sems.at[k]
            )
        )
        stores[-1].start()
        if k + 1 < len(PICK_BLOCKS):
            fill(k + 1)
    for store in stores:
        store.wait()


def pick(perm, planes, last):
    total = perm.shape[1]
    count = planes.shape[0] + 1
    out = jax.ShapeDtypeStruct((total, count * 128), BF16)
    far = pl.BlockSpec(memory_space=pl.ANY)
    scratch = [
        pltpu.VMEM(perm.shape, jnp.int32),
        pltpu.VMEM((count, total, 128), BF16),
        pltpu.VMEM((2, max(PICK_BLOCKS), total), BF16),
        pltpu.VMEM((total, count * 128), BF16),
        pltpu.SemaphoreType.DMA((count + 1,)),
        pltpu.SemaphoreType.DMA((len(PICK_BLOCKS),)),
    ]
    flops = 2 * total * total * count * 128
    return call(pick_kernel, out, flops, 60, scratch, [far] * 3, far)(perm, planes, last)


RESTORE_BLOCKS = (256, 1024, 512, 256)


def restore_kernel(perm_ref, data_ref, planes_hbm, last_hbm, hot_ref, out_ref, sems):
    total = perm_ref.shape[1]
    planes = planes_hbm.shape[0]

    def fill(k):
        start, rows = starts(RESTORE_BLOCKS)[k], RESTORE_BLOCKS[k]
        targets = lax.broadcasted_iota(jnp.int32, (rows, total), 0) + start
        hot = jnp.broadcast_to(perm_ref[...], (rows, total)) == targets
        hot_ref[k % 2, :rows, :] = hot.astype(F32).astype(BF16)

    fill(0)
    stores = []
    for k, (start, rows) in enumerate(zip(starts(RESTORE_BLOCKS), RESTORE_BLOCKS)):
        got = jnp.dot(hot_ref[k % 2, :rows, :], data_ref[...], preferred_element_type=F32).astype(BF16)
        for v in range(planes + 1):
            out_ref[v, start : start + rows, :] = got[:, v * 128 : (v + 1) * 128]
        span = pl.ds(start, rows)
        stores.append(
            pltpu.make_async_copy(
                out_ref.at[pl.ds(0, planes), span, :], planes_hbm.at[:, span, :], sems.at[k, 0]
            )
        )
        stores.append(pltpu.make_async_copy(out_ref.at[planes, span, :], last_hbm.at[span, :], sems.at[k, 1]))
        stores[-2].start()
        stores[-1].start()
        if k + 1 < len(RESTORE_BLOCKS):
            fill(k + 1)
    for store in stores:
        store.wait()


def restore(perm, data):
    total, width = data.shape
    planes = width // 128 - 1
    out = [
        jax.ShapeDtypeStruct((planes, total, 128), BF16),
        jax.ShapeDtypeStruct((total, 128), BF16),
    ]
    near, far = pl.BlockSpec(memory_space=pltpu.VMEM), pl.BlockSpec(memory_space=pl.ANY)
    scratch = [
        pltpu.VMEM((2, max(RESTORE_BLOCKS), total), BF16),
        pltpu.VMEM((planes + 1, total, 128), BF16),
        pltpu.SemaphoreType.DMA((len(RESTORE_BLOCKS), 2)),
    ]
    flops = 2 * total * total * width
    return call(restore_kernel, out, flops, 40, scratch, [near] * 2, [far] * 2)(perm, data)


ADJOINT_ROWS = 512
SCATTER_ROWS = 1024


def two_hot(index_ref, share_ref, start, rows):
    count = index_ref.shape[1]
    block = 256
    first, second, share = index_ref[0:1, :], index_ref[1:2, :], share_ref[...]
    high = jnp.where(first == second, 1.0, share).astype(BF16)
    low = (1.0 - share).astype(BF16)
    targets = lax.broadcasted_iota(jnp.int32, (block, count), 0).astype(F32).astype(BF16)
    spread = lambda row: jnp.broadcast_to(row, (block, count))
    pieces = []
    for at in range(0, rows, block):
        one = spread((first - (start + at)).astype(F32).astype(BF16)) == targets
        two = spread((second - (start + at)).astype(F32).astype(BF16)) == targets
        pieces.append(jnp.where(one, spread(high), jnp.where(two, spread(low), jnp.zeros((), BF16))))
    return pieces[0] if len(pieces) == 1 else jnp.concatenate(pieces, axis=0)


def radiation_kernel(
    data_ref,
    bidx_ref,
    bw_ref,
    cidx_ref,
    cw_ref,
    scale_ref,
    ta_hbm,
    tb_hbm,
    out_ref,
    table_ref,
    sems,
    back_ref,
    coarse_ref,
    tt_ref,
    rows_ref,
    adj_ref,
    mid_ref,
    heat_ref,
):
    bands, width, _ = table_ref.shape
    cols, rows = coarse_ref.shape
    half = bands // 2
    loads = [
        pltpu.make_async_copy(ta_hbm, table_ref.at[pl.ds(0, half)], sems.at[0]),
        pltpu.make_async_copy(tb_hbm, table_ref.at[pl.ds(half, half)], sems.at[1]),
    ]
    for load in loads:
        load.start()

    def adjoint(i, carry):
        start = pl.multiple_of(i * ADJOINT_ROWS, ADJOINT_ROWS)
        matrix = two_hot(bidx_ref, bw_ref, start, ADJOINT_ROWS)
        back_ref[pl.ds(start, ADJOINT_ROWS), :] = matrix
        adj_ref[:, pl.ds(start, ADJOINT_ROWS)] = jnp.dot(
            matrix, data_ref[:, width:], preferred_element_type=F32
        ).T
        return carry

    lax.fori_loop(0, rows // ADJOINT_ROWS, adjoint, 0)
    for load in loads:
        load.wait()

    lifted = jnp.concatenate(
        [(adj_ref[...] * scale_ref[b : b + 1, :]).astype(BF16) for b in range(bands)], axis=0
    )
    tables = jnp.concatenate([table_ref[b] for b in range(bands)], axis=1)
    rows_ref[...] = jnp.dot(tables, lifted, preferred_element_type=F32).astype(BF16)

    def scatter(i, carry):
        start = pl.multiple_of(i * SCATTER_ROWS, SCATTER_ROWS)
        matrix = two_hot(cidx_ref, cw_ref, start, SCATTER_ROWS)
        coarse_ref[pl.ds(start, SCATTER_ROWS), :] = matrix
        got = lax.dot_general(
            rows_ref[...], matrix, (((1,), (1,)), ((), ())), preferred_element_type=F32
        )
        out_ref[pl.ds(start, SCATTER_ROWS), :width] = got.T.astype(BF16)
        per = bands * SCATTER_ROWS // cols
        for k in range(per):
            b = i * per + k
            tt_ref[:, pl.ds(pl.multiple_of(b * width, 128), width)] = table_ref[b].T
        return carry

    lax.fori_loop(0, cols // SCATTER_ROWS, scatter, 0)

    mid_ref[...] = lax.dot_general(
        data_ref[:, :width], coarse_ref[...], (((0,), (0,)), ((), ())), preferred_element_type=F32
    ).astype(BF16)
    lifted = jnp.concatenate(
        [
            mid_ref[...] * jnp.broadcast_to(scale_ref[b : b + 1, :].astype(BF16), mid_ref.shape)
            for b in range(bands)
        ],
        axis=0,
    )
    heat_ref[...] = jnp.dot(tt_ref[...], lifted, preferred_element_type=F32).astype(BF16)
    tendency = jnp.dot(heat_ref[...], back_ref[...], preferred_element_type=F32)
    out_ref[:, width:] = tendency.T.astype(BF16)


def radiation(data, bidx, bw, cidx, cw, scale, ta, tb):
    cols, rows = bw.shape[1], cw.shape[1]
    bands, width, levels = ta.shape
    out = jax.ShapeDtypeStruct((cols, width + levels), BF16)
    flops = 8 * bands * rows * levels * width
    scratch = [
        pltpu.VMEM((2 * bands, width, levels), BF16),
        pltpu.SemaphoreType.DMA((2,)),
        pltpu.VMEM((rows, cols), BF16),
        pltpu.VMEM((cols, rows), BF16),
        pltpu.VMEM((levels, 2 * bands * width), BF16),
        pltpu.VMEM((width, rows), BF16),
        pltpu.VMEM((levels, rows), F32),
        pltpu.VMEM((width, rows), BF16),
        pltpu.VMEM((levels, rows), BF16),
    ]
    near, far = pl.BlockSpec(memory_space=pltpu.VMEM), pl.BlockSpec(memory_space=pl.ANY)
    specs = [near] * 6 + [far] * 2
    kernel = call(radiation_kernel, out, flops, 34, scratch, specs)
    return kernel(data, bidx, bw, cidx, cw, scale, ta, tb)


def gather_four(block, stride):
    lon = lax.axis_size("lon")
    place = lax.rem(lax.axis_index("lon") // stride, 4)
    size = block.shape[0]
    out = jnp.zeros((4 * size,) + block.shape[1:], block.dtype)
    got = [block]
    for shift in (1, 3, 2):
        pairs = []
        for a in range(lon):
            at = a // stride % 4
            pairs.append((a, a + ((at + shift) % 4 - at) * stride))
        got.append(lax.ppermute(block, "lon", pairs))
    for shift, piece in zip((0, 1, 3, 2), got):
        out = lax.dynamic_update_slice_in_dim(
            out, piece, lax.rem(place + 4 - shift, 4) * size, axis=0
        )
    return out


def exchange(values, axes):
    return lax.all_to_all(values, axes, split_axis=0, concat_axis=0, tiled=True)


def local(
    increments,
    cotangent,
    owner_perm,
    coarse_index,
    coarse_weight,
    back_index,
    back_weight,
    lw_scale,
    sw_scale,
    sunlit,
    lw_table,
    sw_table,
):
    lat = lax.axis_size("lat")
    core = lax.rem(lax.axis_index("lat"), 2)
    table = jnp.concatenate([lw_table, sw_table], axis=0)
    bands, _, _, levels = table.shape
    half = bands // 2
    mine = lax.dynamic_slice_in_dim(table, core * half, half, axis=0)
    column = gather_four(mine[None], 1)
    whole = gather_four(column, 4)
    partner = [(a, a + 1 - 2 * (a % 2)) for a in range(lat)]
    other = lax.ppermute(whole, "lat", partner)
    mine, other = (
        t.transpose(1, 2, 0, 3, 4).reshape(half, -1, levels) for t in (whole, other)
    )
    scale = jnp.concatenate([lw_scale, sw_scale * sunlit.astype(F32)[None, :]], axis=0)
    scale = jnp.where(core == 0, scale, jnp.roll(scale, half, axis=0))
    scale = jnp.pad(scale, ((0, 2), (0, 0)))

    cw = coarse_weight[None]
    bw = back_weight[None]
    planes = increments.transpose(1, 0, 2)
    data = pick(owner_perm, planes, cotangent)
    data = exchange(data, ALL)
    back = radiation(data, back_index, bw, coarse_index, cw, scale, mine, other)
    back = exchange(back, ALL)
    gradient, tendency = restore(owner_perm, back)
    return (tendency, gradient.transpose(1, 0, 2))


def solution(mesh):
    in_specs = (
        P(ALL, None, None),
        P(ALL, None),
        P(ALL, None),
        P(None, ALL),
        P(ALL),
        P(None, ALL),
        P(ALL),
        P(None, ALL),
        P(None, ALL),
        P(ALL),
        P(None, None, "lon", None),
        P(None, None, "lon", None),
    )
    out_specs = (P(ALL, None), P(ALL, None, None))
    return jax.shard_map(local, mesh=mesh, in_specs=in_specs, out_specs=out_specs, check_vma=False)
```

```python
import jax
import jax.numpy as jnp
from jax import lax
from jax.experimental import pallas as pl
from jax.experimental.pallas import tpu as pltpu
from jax.sharding import PartitionSpec as P


ALL = ("lat", "lon")
F32 = jnp.float32
BF16 = jnp.bfloat16
MIB = 1 << 20


def call(kernel, out, flops, limit, scratch=(), specs=None, out_specs=None):
    extra = {} if specs is None else {"in_specs": specs}
    if out_specs is not None:
        extra["out_specs"] = out_specs
    return pl.pallas_call(
        kernel,
        out_shape=out,
        **extra,
        scratch_shapes=scratch,
        compiler_params=pltpu.CompilerParams(vmem_limit_bytes=limit * MIB),
        cost_estimate=pl.CostEstimate(flops=flops, bytes_accessed=4 * MIB, transcendentals=0),
    )


PICK_BLOCKS = (256, 512, 1024, 256)


def starts(blocks):
    return [sum(blocks[:k]) for k in range(len(blocks))]


def pick_kernel(perm_hbm, planes_hbm, last_hbm, out_hbm, perm_ref, data_ref, hot_ref, out_ref, in_sems, out_sems):
    total = perm_ref.shape[1]
    planes = planes_hbm.shape[0]
    first = pltpu.make_async_copy(perm_hbm, perm_ref, in_sems.at[planes + 1])
    first.start()
    loads = [pltpu.make_async_copy(planes_hbm.at[v], data_ref.at[v], in_sems.at[v]) for v in range(planes)]
    loads.append(pltpu.make_async_copy(last_hbm, data_ref.at[planes], in_sems.at[planes]))
    for load in loads:
        load.start()
    first.wait()

    def fill(k):
        start, rows = starts(PICK_BLOCKS)[k], PICK_BLOCKS[k]
        index = jnp.transpose(jnp.broadcast_to(perm_ref[:, start : start + rows], (128, rows)))
        lanes = lax.broadcasted_iota(jnp.int32, (rows, total), 1)
        hot = jnp.concatenate([index] * (total // 128), axis=1) == lanes
        hot_ref[k % 2, :rows, :] = hot.astype(F32).astype(BF16)

    fill(0)
    stores = []
    for k, (start, rows) in enumerate(zip(starts(PICK_BLOCKS), PICK_BLOCKS)):
        step = 2 if k == 0 else planes + 1
        for v in range(0, planes + 1, step):
            if k == 0:
                for load in loads[v : v + step]:
                    load.wait()
            data = jnp.concatenate([data_ref[u] for u in range(v, v + step)], axis=1)
            got = jnp.dot(hot_ref[k % 2, :rows, :], data, preferred_element_type=F32)
            out_ref[start : start + rows, v * 128 : (v + step) * 128] = got.astype(BF16)
        stores.append(
            pltpu.make_async_copy(
                out_ref.at[pl.ds(start, rows), :], out_hbm.at[pl.ds(start, rows), :], out_sems.at[k]
            )
        )
        stores[-1].start()
        if k + 1 < len(PICK_BLOCKS):
            fill(k + 1)
    for store in stores:
        store.wait()


def pick(perm, planes, last):
    total = perm.shape[1]
    count = planes.shape[0] + 1
    out = jax.ShapeDtypeStruct((total, count * 128), BF16)
    far = pl.BlockSpec(memory_space=pl.ANY)
    scratch = [
        pltpu.VMEM(perm.shape, jnp.int32),
        pltpu.VMEM((count, total, 128), BF16),
        pltpu.VMEM((2, max(PICK_BLOCKS), total), BF16),
        pltpu.VMEM((total, count * 128), BF16),
        pltpu.SemaphoreType.DMA((count + 1,)),
        pltpu.SemaphoreType.DMA((len(PICK_BLOCKS),)),
    ]
    flops = 2 * total * total * count * 128
    return call(pick_kernel, out, flops, 60, scratch, [far] * 3, far)(perm, planes, last)


RESTORE_BLOCKS = (256, 1024, 512, 256)


def restore_kernel(perm_ref, data_ref, planes_hbm, last_hbm, hot_ref, out_ref, sems):
    total = perm_ref.shape[1]
    planes = planes_hbm.shape[0]

    def fill(k):
        start, rows = starts(RESTORE_BLOCKS)[k], RESTORE_BLOCKS[k]
        targets = lax.broadcasted_iota(jnp.int32, (rows, total), 0) + start
        hot = jnp.broadcast_to(perm_ref[...], (rows, total)) == targets
        hot_ref[k % 2, :rows, :] = hot.astype(F32).astype(BF16)

    fill(0)
    stores = []
    for k, (start, rows) in enumerate(zip(starts(RESTORE_BLOCKS), RESTORE_BLOCKS)):
        got = jnp.dot(hot_ref[k % 2, :rows, :], data_ref[...], preferred_element_type=F32).astype(BF16)
        for v in range(planes + 1):
            out_ref[v, start : start + rows, :] = got[:, v * 128 : (v + 1) * 128]
        span = pl.ds(start, rows)
        stores.append(
            pltpu.make_async_copy(
                out_ref.at[pl.ds(0, planes), span, :], planes_hbm.at[:, span, :], sems.at[k, 0]
            )
        )
        stores.append(pltpu.make_async_copy(out_ref.at[planes, span, :], last_hbm.at[span, :], sems.at[k, 1]))
        stores[-2].start()
        stores[-1].start()
        if k + 1 < len(RESTORE_BLOCKS):
            fill(k + 1)
    for store in stores:
        store.wait()


def restore(perm, data):
    total, width = data.shape
    planes = width // 128 - 1
    out = [
        jax.ShapeDtypeStruct((planes, total, 128), BF16),
        jax.ShapeDtypeStruct((total, 128), BF16),
    ]
    near, far = pl.BlockSpec(memory_space=pltpu.VMEM), pl.BlockSpec(memory_space=pl.ANY)
    scratch = [
        pltpu.VMEM((2, max(RESTORE_BLOCKS), total), BF16),
        pltpu.VMEM((planes + 1, total, 128), BF16),
        pltpu.SemaphoreType.DMA((len(RESTORE_BLOCKS), 2)),
    ]
    flops = 2 * total * total * width
    return call(restore_kernel, out, flops, 40, scratch, [near] * 2, [far] * 2)(perm, data)


ADJOINT_ROWS = 512
SCATTER_ROWS = 1024


def two_hot(index_ref, share_ref, start, rows):
    count = index_ref.shape[1]
    block = 256
    first, second, share = index_ref[0:1, :], index_ref[1:2, :], share_ref[...]
    high = jnp.where(first == second, 1.0, share).astype(BF16)
    low = (1.0 - share).astype(BF16)
    targets = lax.broadcasted_iota(jnp.int32, (block, count), 0).astype(F32).astype(BF16)
    spread = lambda row: jnp.broadcast_to(row, (block, count))
    pieces = []
    for at in range(0, rows, block):
        one = spread((first - (start + at)).astype(F32).astype(BF16)) == targets
        two = spread((second - (start + at)).astype(F32).astype(BF16)) == targets
        pieces.append(jnp.where(one, spread(high), jnp.where(two, spread(low), jnp.zeros((), BF16))))
    return pieces[0] if len(pieces) == 1 else jnp.concatenate(pieces, axis=0)


def radiation_kernel(
    data_ref,
    bidx_ref,
    bw_ref,
    cidx_ref,
    cw_ref,
    scale_ref,
    ta_hbm,
    tb_hbm,
    out_ref,
    table_ref,
    sems,
    back_ref,
    coarse_ref,
    tt_ref,
    rows_ref,
    adj_ref,
    mid_ref,
    heat_ref,
):
    bands, width, _ = table_ref.shape
    cols, rows = coarse_ref.shape
    half = bands // 2
    loads = [
        pltpu.make_async_copy(ta_hbm, table_ref.at[pl.ds(0, half)], sems.at[0]),
        pltpu.make_async_copy(tb_hbm, table_ref.at[pl.ds(half, half)], sems.at[1]),
    ]
    for load in loads:
        load.start()

    def adjoint(i, carry):
        start = pl.multiple_of(i * ADJOINT_ROWS, ADJOINT_ROWS)
        matrix = two_hot(bidx_ref, bw_ref, start, ADJOINT_ROWS)
        back_ref[pl.ds(start, ADJOINT_ROWS), :] = matrix
        adj_ref[:, pl.ds(start, ADJOINT_ROWS)] = jnp.dot(
            matrix, data_ref[:, width:], preferred_element_type=F32
        ).T
        return carry

    lax.fori_loop(0, rows // ADJOINT_ROWS, adjoint, 0)
    for load in loads:
        load.wait()

    lifted = jnp.concatenate(
        [(adj_ref[...] * scale_ref[b : b + 1, :]).astype(BF16) for b in range(bands)], axis=0
    )
    tables = jnp.concatenate([table_ref[b] for b in range(bands)], axis=1)
    rows_ref[...] = jnp.dot(tables, lifted, preferred_element_type=F32).astype(BF16)

    def scatter(i, carry):
        start = pl.multiple_of(i * SCATTER_ROWS, SCATTER_ROWS)
        matrix = two_hot(cidx_ref, cw_ref, start, SCATTER_ROWS)
        coarse_ref[pl.ds(start, SCATTER_ROWS), :] = matrix
        got = lax.dot_general(
            rows_ref[...], matrix, (((1,), (1,)), ((), ())), preferred_element_type=F32
        )
        out_ref[pl.ds(start, SCATTER_ROWS), :width] = got.T.astype(BF16)
        per = bands * SCATTER_ROWS // cols
        for k in range(per):
            b = i * per + k
            tt_ref[:, pl.ds(pl.multiple_of(b * width, 128), width)] = table_ref[b].T
        return carry

    lax.fori_loop(0, cols // SCATTER_ROWS, scatter, 0)

    mid_ref[...] = lax.dot_general(
        data_ref[:, :width], coarse_ref[...], (((0,), (0,)), ((), ())), preferred_element_type=F32
    ).astype(BF16)
    lifted = jnp.concatenate(
        [
            mid_ref[...] * jnp.broadcast_to(scale_ref[b : b + 1, :].astype(BF16), mid_ref.shape)
            for b in range(bands)
        ],
        axis=0,
    )
    heat_ref[...] = jnp.dot(tt_ref[...], lifted, preferred_element_type=F32).astype(BF16)
    tendency = jnp.dot(heat_ref[...], back_ref[...], preferred_element_type=F32)
    out_ref[:, width:] = tendency.T.astype(BF16)


def radiation(data, bidx, bw, cidx, cw, scale, ta, tb):
    cols, rows = bw.shape[1], cw.shape[1]
    bands, width, levels = ta.shape
    out = jax.ShapeDtypeStruct((cols, width + levels), BF16)
    flops = 8 * bands * rows * levels * width
    scratch = [
        pltpu.VMEM((2 * bands, width, levels), BF16),
        pltpu.SemaphoreType.DMA((2,)),
        pltpu.VMEM((rows, cols), BF16),
        pltpu.VMEM((cols, rows), BF16),
        pltpu.VMEM((levels, 2 * bands * width), BF16),
        pltpu.VMEM((width, rows), BF16),
        pltpu.VMEM((levels, rows), F32),
        pltpu.VMEM((width, rows), BF16),
        pltpu.VMEM((levels, rows), BF16),
    ]
    near, far = pl.BlockSpec(memory_space=pltpu.VMEM), pl.BlockSpec(memory_space=pl.ANY)
    specs = [near] * 6 + [far] * 2
    kernel = call(radiation_kernel, out, flops, 34, scratch, specs)
    return kernel(data, bidx, bw, cidx, cw, scale, ta, tb)


def gather_four(block, stride):
    lon = lax.axis_size("lon")
    place = lax.rem(lax.axis_index("lon") // stride, 4)
    size = block.shape[0]
    out = jnp.zeros((4 * size,) + block.shape[1:], block.dtype)
    got = [block]
    for shift in (1, 3, 2):
        pairs = []
        for a in range(lon):
            at = a // stride % 4
            pairs.append((a, a + ((at + shift) % 4 - at) * stride))
        got.append(lax.ppermute(block, "lon", pairs))
    for shift, piece in zip((0, 1, 3, 2), got):
        out = lax.dynamic_update_slice_in_dim(
            out, piece, lax.rem(place + 4 - shift, 4) * size, axis=0
        )
    return out


def exchange(values, axes):
    return lax.all_to_all(values, axes, split_axis=0, concat_axis=0, tiled=True)


def local(
    increments,
    cotangent,
    owner_perm,
    coarse_index,
    coarse_weight,
    back_index,
    back_weight,
    lw_scale,
    sw_scale,
    sunlit,
    lw_table,
    sw_table,
):
    lat = lax.axis_size("lat")
    core = lax.rem(lax.axis_index("lat"), 2)
    table = jnp.concatenate([lw_table, sw_table], axis=0)
    bands, _, _, levels = table.shape
    half = bands // 2
    mine = lax.dynamic_slice_in_dim(table, core * half, half, axis=0)
    column = gather_four(mine[None], 1)
    whole = gather_four(column, 4)
    partner = [(a, a + 1 - 2 * (a % 2)) for a in range(lat)]
    other = lax.ppermute(whole, "lat", partner)
    mine, other = (
        t.transpose(1, 2, 0, 3, 4).reshape(half, -1, levels) for t in (whole, other)
    )
    scale = jnp.concatenate([lw_scale, sw_scale * sunlit.astype(F32)[None, :]], axis=0)
    scale = jnp.where(core == 0, scale, jnp.roll(scale, half, axis=0))
    scale = jnp.pad(scale, ((0, 2), (0, 0)))

    cw = coarse_weight[None]
    bw = back_weight[None]
    planes = increments.transpose(1, 0, 2)
    data = pick(owner_perm, planes, cotangent)
    data = exchange(data, ALL)
    back = radiation(data, back_index, bw, coarse_index, cw, scale, mine, other)
    back = exchange(back, ALL)
    gradient, tendency = restore(owner_perm, back)
    return (tendency, gradient.transpose(1, 0, 2))


def solution(mesh):
    in_specs = (
        P(ALL, None, None),
        P(ALL, None),
        P(ALL, None),
        P(None, ALL),
        P(ALL),
        P(None, ALL),
        P(ALL),
        P(None, ALL),
        P(None, ALL),
        P(ALL),
        P(None, None, "lon", None),
        P(None, None, "lon", None),
    )
    out_specs = (P(ALL, None), P(ALL, None, None))
    return jax.shard_map(local, mesh=mesh, in_specs=in_specs, out_specs=out_specs, check_vma=False)
```
